256 devices in a mesh: groups: 2 (over z), seq: 16 (over y, core), head: 8 (over x).
Axes of the slice: x: 8, y: 8, z: 2, core: 2. Of those that a mesh axis runs over, the one named last changes fastest.
The devices are a block of a 8x8x16 slice.
Arguments:
- query: bfloat16 [32, 16, 1024], P('groups', None, 'head'), parts along dimension 0, may hold values from -6 to 6, as said below
- new_key: bfloat16 [32, 16, 1024], P('groups', None, 'head'), parts along dimension 0, may hold values from -6 to 6
- new_value: bfloat16 [32, 16, 1024], P('groups', None, 'head'), parts along dimension 0, may hold values from -6 to 6
- keys: bfloat16 [32, 16384, 1024], P('groups', 'seq', 'head'), parts along dimension 0, may hold values from -6 to 6, as said below
- values: bfloat16 [32, 16384, 1024], P('groups', 'seq', 'head'), parts along dimension 0, may hold values from -6 to 6
- lengths: int32 [32], P('groups'), parts along dimension 0, may hold values from 2 to 16384
- time_bucket: int32 [32, 16384], P('groups', 'seq'), parts along dimension 0, may hold values from 0 to 63
- action: int32 [32, 16384], P('groups', 'seq'), parts along dimension 0, may hold values from 0 to 15
- time_bias: float32 [64, 8], P(None, 'head'), may hold values from -0.25 to 0.25
- action_bias: float32 [16, 8], P(None, 'head'), may hold values from -0.25 to 0.25
- gate: bfloat16 [32, 16, 1024], P('groups', None, 'head'), parts along dimension 0, may hold values from -6 to 6
- norm_gain: float32 [1024], P('head'), may hold values from 0.1 to 1.9
- w_out: bfloat16 [1024, 1024], P('head'), may hold values from -0.1875 to 0.1875
Outputs:
- output: bfloat16 [32, 16, 1024], P(('groups', 'seq'), None, 'head'), parts along dimension 0
The draws below stay inside these ranges and needn't reach their ends.
There are 2 independent parts, one for each index of `groups`. The reference program is written for one: setup_inputs(seed, part) draws one part's arguments, and reference() takes and returns one part's arrays. A program takes and returns all parts, laid end to end along the dimension named above; an argument that names none is the same for every part. Nothing has to cross between parts.
Inputs may be any that keep to these rules, and one draw needn't show every extreme that they name: `query`: queries of order one; some users' queries may be large and equal to some of their keys. `keys`: keys of order one.
All inputs are finite; a program needn't handle non-finite values.
Results may differ from the reference program's by a relative error of at most 0.0056.
Values sent between devices are 32-bit elements; how exact they have to be, the bound alone decides.
A program may use at most 64 MiB of HBM per device.

```python
import math
import jax
import jax.numpy as jnp
from jax import lax

USERS = 16
CANDS = 16
S_DEV = 1024
HEADS = 8
DH = 128
D_MODEL = 1024
BUCKETS = 64
ACTIONS = 16
HISTORY = 16384
N_SEQ = 16


def draw_query(key, part):
    result = jax.random.truncated_normal(jax.random.fold_in(key, 1), -6.0, 6.0, (USERS, CANDS, HEADS * DH), jnp.float32)
    return result.astype(jnp.bfloat16)


def draw_keys(key, part):
    result = jax.random.truncated_normal(jax.random.fold_in(key, 2), -6.0, 6.0, (USERS, HISTORY, HEADS * DH), jnp.float32)
    return result.astype(jnp.bfloat16)


def plant(values, key, smallest, top_value):
    place = [jax.random.randint(jax.random.fold_in(key, axis), (), 0, length) for axis, length in enumerate(values.shape)]
    widest = values.shape.index(max(values.shape))
    beside = place[:widest] + [(place[widest] + 1) % values.shape[widest]] + place[widest + 1:]
    return values.at[tuple(place)].set(smallest).at[tuple(beside)].set(top_value)


def block_levels(key, dims, split, least, largest):
    def one(dim, blocks):
        steps = jax.random.uniform(jax.random.fold_in(jax.random.fold_in(key, 6), dim), (blocks,), jnp.float32, least / len(split), largest / len(split))
        return jnp.repeat(jnp.exp(steps), dims[dim] // blocks).reshape((-1,) + (1,) * (len(dims) - dim - 1))

    gain = one(*split[0])
    for cut in split[1:]:
        gain = gain * one(*cut)
    return gain


def noise(stream_key, extent, scale, bound, split=(), held_as=jnp.bfloat16):
    values = scale * jax.random.normal(stream_key, extent, jnp.float32)
    if split:
        values = values * block_levels(stream_key, extent, split, -0.22, 0.18)
    return jnp.clip(values, -bound, bound).astype(held_as)


def setup_inputs(seed: int = 0, part: int = 0) -> dict:
    splits = jax.random.split(jax.random.key(seed), 14)
    own_keys = jax.random.split(jax.random.fold_in(splits[13], part), 14)
    return {
        "query": draw_query(jax.random.fold_in(jax.random.fold_in(splits[13], part), 71), part),
        "new_key": noise(own_keys[1], (USERS, CANDS, HEADS * DH), 1.0, 6.0, ((2, 8),)),
        "new_value": noise(own_keys[2], (USERS, CANDS, HEADS * DH), 1.0, 6.0, ((2, 8),)),
        "keys": draw_keys(jax.random.fold_in(jax.random.fold_in(splits[13], part), 71), part),
        "values": noise(own_keys[4], (USERS, HISTORY, HEADS * DH), 1.0, 6.0, ((1, 16), (2, 8))),
        "lengths": plant(jax.random.randint(own_keys[5], (USERS,), 2, HISTORY + 1), jax.random.fold_in(own_keys[5], 1), 2, HISTORY).astype(jnp.int32),
        "time_bucket": plant(jax.random.randint(own_keys[6], (USERS, HISTORY), 0, BUCKETS), jax.random.fold_in(own_keys[6], 1), 0, BUCKETS - 1).astype(jnp.int32),
        "action": plant(jax.random.randint(own_keys[7], (USERS, HISTORY), 0, ACTIONS), jax.random.fold_in(own_keys[7], 1), 0, ACTIONS - 1).astype(jnp.int32),
        "time_bias": jnp.clip(jax.random.uniform(splits[8], (BUCKETS, HEADS), jnp.float32, -0.25, 0.25) * block_levels(splits[8], (BUCKETS, HEADS), ((1, 8),), -0.4, 0.0), -0.25, 0.25),
        "action_bias": jnp.clip(jax.random.uniform(splits[9], (ACTIONS, HEADS), jnp.float32, -0.25, 0.25) * block_levels(splits[9], (ACTIONS, HEADS), ((1, 8),), -0.4, 0.0), -0.25, 0.25),
        "gate": noise(own_keys[10], (USERS, CANDS, HEADS * DH), 1.0, 6.0, ((2, 8),)),
        "norm_gain": jnp.clip(1.0 + 0.18 * jax.random.normal(splits[11], (HEADS * DH,), jnp.float32), 0.1, 1.9),
        "w_out": noise(splits[12], (HEADS * DH, D_MODEL), (HEADS * DH) ** -0.5, 0.1875, ((0, 8),)),
    }


def reference(query, new_key, new_value, keys, values, lengths, time_bucket, action, time_bias, action_bias, gate, norm_gain, w_out):
    user_count = keys.shape[0]
    cand_count = query.shape[1]
    head_count = HEADS
    head_size = DH
    score_scale = 1.0 / math.sqrt(head_size)
    query_heads = query.astype(jnp.float32).reshape(user_count, cand_count, head_count, head_size)

    def one_block(block_index):
        first = (block_index * S_DEV).astype(jnp.int32)
        key_block = lax.dynamic_slice_in_dim(keys, first, S_DEV, 1).astype(jnp.float32).reshape(user_count, S_DEV, head_count, head_size)
        value_block = lax.dynamic_slice_in_dim(values, first, S_DEV, 1).astype(jnp.float32).reshape(user_count, S_DEV, head_count, head_size)
        bucket_block = lax.dynamic_slice_in_dim(time_bucket, first, S_DEV, 1)
        action_block = lax.dynamic_slice_in_dim(action, first, S_DEV, 1)
        scores = jnp.einsum('uchd,ushd->uchs', query_heads, key_block) * score_scale
        biases = jnp.transpose(time_bias[bucket_block], (0, 2, 1)) + jnp.transpose(action_bias[action_block], (0, 2, 1))
        scores = scores + biases[:, None]
        position = first + jnp.arange(S_DEV, dtype=jnp.int32)
        valid = position[None, None, None, :] < lengths[:, None, None, None]
        block_max = lax.optimization_barrier(jnp.max(jnp.where(valid, scores, -1e+30), axis=-1))
        weights = jnp.where(valid, jnp.exp(scores - block_max[..., None]), 0.0)
        block_sum = lax.optimization_barrier(jnp.sum(weights, axis=-1))
        rounded = weights.astype(jnp.bfloat16).astype(jnp.float32)
        block_acc = jnp.einsum('uchs,ushd->uchd', rounded, value_block)
        return (block_max, block_sum, block_acc)
    maxima, sums, accs = lax.map(one_block, jnp.arange(N_SEQ, dtype=jnp.int32))
    own = lax.optimization_barrier(jnp.sum(query_heads * new_key.astype(jnp.float32).reshape(user_count, cand_count, head_count, head_size), axis=-1)) * score_scale
    overall = jnp.maximum(lax.optimization_barrier(jnp.max(maxima, axis=0)), own)
    factors = jnp.exp(maxima - overall[None])
    own_factor = jnp.exp(own - overall)
    numer = lax.optimization_barrier(jnp.sum(factors[..., None] * accs, axis=0)) + own_factor[..., None] * new_value.astype(jnp.float32).reshape(user_count, cand_count, head_count, head_size)
    denom = lax.optimization_barrier(jnp.sum(factors * sums, axis=0)) + own_factor
    attended = numer / denom[..., None]
    square_sum = lax.optimization_barrier(jnp.sum(jnp.square(attended), axis=(2, 3)))
    gate_heads = gate.astype(jnp.float32).reshape(user_count, cand_count, head_count, head_size)
    hidden = (attended * norm_gain.reshape(head_count, head_size) * jax.nn.silu(gate_heads)).astype(jnp.bfloat16)
    hidden = hidden.reshape(user_count * cand_count, head_count * head_size)
    projected = jnp.dot(hidden, w_out, preferred_element_type=jnp.float32).reshape(user_count, cand_count, -1)
    factor = 1.0 / jnp.sqrt(square_sum / (head_count * head_size) + 1e-06)
    return (projected * factor[:, :, None]).astype(jnp.bfloat16)
```

```python
import functools
import math

import jax
import jax.numpy as jnp
from jax import lax
from jax.experimental import pallas as pl
from jax.experimental.pallas import tpu as pltpu
from jax.sharding import PartitionSpec as P

MESH = pl.DeviceIdType.MESH
LOG2E = math.log2(math.e)
LANES = 128
GROUP = 4


def far_first(count):
    return sorted(range(count), key=lambda d: (-min(d, count - d), d))


def table_lookup(table, index):
    rows = jnp.broadcast_to(table, (8, table.shape[1]))
    if table.shape[1] < LANES:
        rows = jnp.concatenate(
            [rows, jnp.zeros((8, LANES - table.shape[1]), rows.dtype)], axis=1
        )
    blocks = []
    for r in range(0, index.shape[0], 8):
        blocks.append(
            jnp.concatenate(
                [
                    jnp.take_along_axis(rows, index[r : r + 8, c : c + LANES], axis=1)
                    for c in range(0, index.shape[1], LANES)
                ],
                axis=1,
            )
        )
    return jnp.concatenate(blocks, axis=0)


def kernel(
    query,
    new_key,
    new_value,
    keys,
    values,
    lengths,
    time_bucket,
    action,
    time_bias,
    action_bias,
    gate,
    norm_gain,
    w_out,
    out,
    q_buf,
    nk_buf,
    nv_buf,
    k_buf,
    v_buf,
    len_buf,
    tb_buf,
    ac_buf,
    tbias_buf,
    abias_buf,
    gate_buf,
    gain_buf,
    w_buf,
    bias_buf,
    send1,
    recv1,
    send2,
    recv2,
    in_sem,
    k_sem,
    v_sem,
    send_sem1,
    recv_sem1,
    send_sem2,
    recv_sem2,
):
    n_seq = lax.axis_size("seq")
    n_head = lax.axis_size("head")
    me = lax.axis_index("seq")
    my_head = lax.axis_index("head")
    users, cands, width = query.shape
    block_len = keys.shape[1]
    half = cands // 2
    scale = LOG2E / math.sqrt(width)
    order = far_first(n_seq)

    def seq_peer(d):
        return lax.rem(me + d, n_seq)

    def head_peer(e):
        return lax.rem(my_head + e, n_head)

    small = [
        (lengths, len_buf),
        (time_bias, tbias_buf),
        (action_bias, abias_buf),
        (time_bucket, tb_buf),
        (action, ac_buf),
        (query, q_buf),
        (new_key.at[me], nk_buf),
        (new_value.at[me], nv_buf),
        (gate.at[me], gate_buf),
        (norm_gain, gain_buf),
        (w_out, w_buf),
    ]
    loads = [
        pltpu.make_async_copy(src, dst, in_sem.at[i]) for i, (src, dst) in enumerate(small)
    ]
    k_loads, v_loads = {}, {}
    for d in order:
        user = seq_peer(d)
        k_loads[d] = pltpu.make_async_copy(keys.at[user], k_buf.at[d], k_sem.at[d])
        v_loads[d] = pltpu.make_async_copy(values.at[user], v_buf.at[d], v_sem.at[d])
    for load in loads[:6]:
        load.start()
    for d in order:
        k_loads[d].start()
        v_loads[d].start()
    for load in loads[6:]:
        load.start()

    barrier = pltpu.get_barrier_semaphore()
    for d in order[:-1]:
        pl.semaphore_signal(barrier, inc=1, device_id={"seq": seq_peer(d)}, device_id_type=MESH)
    for e in range(1, n_head):
        pl.semaphore_signal(barrier, inc=1, device_id={"head": head_peer(e)}, device_id_type=MESH)

    for load in loads[:6]:
        load.wait()
    biases = table_lookup(tbias_buf[...], tb_buf[...]) + table_lookup(abias_buf[...], ac_buf[...])
    row = lax.broadcasted_iota(jnp.int32, (users, block_len), 0)
    limit = jnp.zeros((users, block_len), jnp.int32)
    for u in range(users):
        limit = jnp.where(row == u, len_buf[u], limit)
    position = me * block_len + lax.broadcasted_iota(jnp.int32, (users, block_len), 1)
    bias_buf[...] = jnp.where(position < limit, biases * LOG2E, -1e30)

    lane = lax.broadcasted_iota(jnp.int32, (half, LANES), 1)

    def attend(d):
        user = seq_peer(d)
        scores = (
            lax.dot_general(
                q_buf[user],
                k_buf[d],
                (((1,), (1,)), ((), ())),
                preferred_element_type=jnp.float32,
            )
            * scale
            + bias_buf[pl.ds(user, 1), :]
        )
        top = jnp.max(scores, axis=1, keepdims=True)
        weights = jnp.exp2(scores - top)
        total = jnp.sum(weights, axis=1, keepdims=True)
        acc = jnp.dot(
            weights.astype(jnp.bfloat16), v_buf[d], preferred_element_type=jnp.float32
        )
        packed = jnp.where(
            lane < 32,
            top[:half],
            jnp.where(lane < 64, top[half:], jnp.where(lane < 96, total[:half], total[half:])),
        )
        return acc, packed

    sends = []
    for first in range(0, n_seq, GROUP):
        group = order[first : first + GROUP]
        for d in group:
            k_loads[d].wait()
            v_loads[d].wait()
        for d in group:
            acc, packed = attend(d)
            place = recv1 if d == 0 else send1
            place[d, 0:cands] = acc
            place[d, cands : cands + half] = packed
        if first == 0:
            pl.semaphore_wait(barrier, n_seq - 1 + n_head - 1)
        for d in group:
            if d:
                copy = pltpu.make_async_remote_copy(
                    src_ref=send1.at[d],
                    dst_ref=recv1.at[d],
                    send_sem=send_sem1.at[d],
                    recv_sem=recv_sem1.at[d],
                    device_id={"seq": seq_peer(d)},
                    device_id_type=MESH,
                )
                copy.start()
                sends.append(copy)

    for load in loads[6:]:
        load.wait()
    own_query = q_buf[me].astype(jnp.float32)
    own = jnp.sum(own_query * nk_buf[...].astype(jnp.float32), axis=1, keepdims=True) * scale
    own = jnp.where(lane < 32, own[:half], own[half:])
    gate_rows = gate_buf[...].astype(jnp.float32)
    gated = gain_buf[...] * (gate_rows / (1.0 + jnp.exp(-gate_rows)))
    own_value = nv_buf[...].astype(jnp.float32)

    for copy in sends:
        copy.wait_recv()
    marks = [recv1[d, cands : cands + half] for d in range(n_seq)]
    overall = own
    for mark in marks:
        overall = jnp.maximum(overall, mark)
    factor = jnp.exp2(own - overall)

    def spread(values):
        return jnp.concatenate(
            [
                jnp.broadcast_to(values[:, 0:1], (half, width)),
                jnp.broadcast_to(values[:, 32:33], (half, width)),
            ],
            axis=0,
        )

    denom = factor
    numer = spread(factor) * own_value
    for d, mark in enumerate(marks):
        factor = jnp.exp2(mark - overall)
        denom = denom + factor * pltpu.roll(mark, 64, 1)
        numer = numer + spread(factor) * recv1[d, 0:cands]
    attended = numer / spread(denom)
    squares = jnp.sum(attended * attended, axis=1, keepdims=True)
    hidden = (attended * gated).astype(jnp.bfloat16)
    squares = jnp.where(lane < 32, squares[:half], squares[half:])
    for h in range(n_head):
        send2[h, 0:cands] = jnp.dot(
            hidden, w_buf[:, h * width : (h + 1) * width], preferred_element_type=jnp.float32
        )
        send2[h, cands : cands + half] = squares
    sends2 = []
    for e in far_first(n_head)[:-1]:
        copy = pltpu.make_async_remote_copy(
            src_ref=send2.at[head_peer(e)],
            dst_ref=recv2.at[e],
            send_sem=send_sem2.at[e],
            recv_sem=recv_sem2.at[e],
            device_id={"head": head_peer(e)},
            device_id_type=MESH,
        )
        copy.start()
        sends2.append(copy)
    whole = send2[my_head]
    for copy in sends2:
        copy.wait_recv()
    for e in range(1, n_head):
        whole = whole + recv2[e]
    square_sum = spread(whole[cands : cands + half])
    scaled = whole[0:cands] * (1.0 / jnp.sqrt(square_sum / (width * n_head) + 1e-06))
    out[0] = scaled.astype(out.dtype)
    for copy in sends + sends2:
        copy.wait_send()


def body(
    query,
    new_key,
    new_value,
    keys,
    values,
    lengths,
    time_bucket,
    action,
    time_bias,
    action_bias,
    gate,
    norm_gain,
    w_out,
):
    users, block_len, width = keys.shape
    cands = query.shape[1]
    n_seq, n_head = lax.axis_size("seq"), lax.axis_size("head")
    assert users == n_seq and width == LANES and w_out.shape[1] == n_head * width
    tile = cands + cands // 2
    bf16, f32, i32 = jnp.bfloat16, jnp.float32, jnp.int32
    vmem, dma = pltpu.VMEM, pltpu.SemaphoreType.DMA
    buckets, actions = time_bias.shape[0], action_bias.shape[0]
    return pl.pallas_call(
        kernel,
        name="decode",
        out_shape=jax.ShapeDtypeStruct((users // n_seq, cands, width), bf16),
        in_specs=[pl.BlockSpec(memory_space=pl.ANY)] * 13,
        out_specs=pl.BlockSpec(memory_space=vmem),
        scratch_shapes=[
            vmem((users, cands, width), bf16),
            vmem((cands, width), bf16),
            vmem((cands, width), bf16),
            vmem((users, block_len, width), bf16),
            vmem((users, block_len, width), bf16),
            pltpu.SMEM((users,), i32),
            vmem((users, block_len), i32),
            vmem((users, block_len), i32),
            vmem((1, buckets), f32),
            vmem((1, actions), f32),
            vmem((cands, width), bf16),
            vmem((1, width), f32),
            vmem((width, n_head * width), bf16),
            vmem((users, block_len), f32),
            vmem((n_seq, tile, width), f32),
            vmem((n_seq, tile, width), f32),
            vmem((n_head, tile, width), f32),
            vmem((n_head, tile, width), f32),
            dma((11,)),
            dma((n_seq,)),
            dma((n_seq,)),
            dma((n_seq,)),
            dma((n_seq,)),
            dma((n_head,)),
            dma((n_head,)),
        ],
        compiler_params=pltpu.CompilerParams(collective_id=0, has_side_effects=True),
    )(
        query,
        new_key,
        new_value,
        keys,
        values,
        lengths,
        time_bucket,
        action,
        time_bias.reshape(1, buckets),
        action_bias.reshape(1, actions),
        gate,
        norm_gain.reshape(1, width),
        w_out,
    )


def solution(mesh):
    placed = (
        P("groups", None, "head"),
        P("groups", None, "head"),
        P("groups", None, "head"),
        P("groups", "seq", "head"),
        P("groups", "seq", "head"),
        P("groups"),
        P("groups", "seq"),
        P("groups", "seq"),
        P(None, "head"),
        P(None, "head"),
        P("groups", None, "head"),
        P("head"),
        P("head", None),
    )
    return jax.shard_map(
        body,
        mesh=mesh,
        in_specs=placed,
        out_specs=P(("groups", "seq"), None, "head"),
        check_vma=False,
    )
```

```python
import math

import jax
import jax.numpy as jnp
from jax import lax
from jax.experimental import pallas as pl
from jax.experimental.pallas import tpu as pltpu
from jax.sharding import PartitionSpec as P

MESH = pl.DeviceIdType.MESH
LOG2E = math.log2(math.e)
LANES = 128
PAIR = 2
SPAN = 2


def far_first(count):
    return sorted(range(count), key=lambda d: (-min(d, count - d), d))


def lane_table(table):
    rows = jnp.broadcast_to(table, (8, table.shape[1]))
    rest = LANES - table.shape[1]
    if rest:
        rows = jnp.concatenate([rows, jnp.zeros((8, rest), rows.dtype)], axis=1)
    return rows


def kernel(
    query,
    new_key,
    new_value,
    keys,
    values,
    lengths,
    time_bucket,
    action,
    time_bias,
    action_bias,
    gate,
    norm_gain,
    w_out,
    out,
    q_buf,
    nk_buf,
    nv_buf,
    k_buf,
    v_buf,
    len_buf,
    tb_buf,
    ac_buf,
    tbias_buf,
    abias_buf,
    gate_buf,
    gain_buf,
    w_buf,
    bias_buf,
    score_buf,
    send1,
    recv1,
    send2,
    recv2,
    send3,
    recv3,
    in_sem,
    k_sem,
    v_sem,
    send_sem1,
    recv_sem1,
    send_sem2,
    recv_sem2,
    send_sem3,
    recv_sem3,
):
    n_seq = lax.axis_size("seq")
    n_head = lax.axis_size("head")
    n_chip = n_seq // PAIR
    me = lax.axis_index("seq")
    chip, core = lax.div(me, PAIR), lax.rem(me, PAIR)
    my_head = lax.axis_index("head")
    users, cands, width = query.shape
    block_len = keys.shape[1]
    pair_rows = PAIR * cands
    scale = LOG2E / math.sqrt(width)
    order = far_first(n_chip)
    f32, bf16 = jnp.float32, jnp.bfloat16

    def chip_at(e):
        return lax.rem(chip + e, n_chip)

    def head_at(e):
        return lax.rem(my_head + e, n_head)

    def pair_of(source, e):
        return source.at[pl.ds(chip_at(e) * PAIR, PAIR)]

    early = [
        (lengths, len_buf),
        (time_bias, tbias_buf),
        (action_bias, abias_buf),
        (time_bucket, tb_buf),
        (action, ac_buf),
        (query, q_buf),
    ]
    late = [
        (pair_of(new_key, 0), nk_buf),
        (pair_of(new_value, 0), nv_buf),
        (pair_of(gate, 0), gate_buf),
        (norm_gain, gain_buf),
        (w_out, w_buf),
    ]
    loads = [
        pltpu.make_async_copy(src, dst, in_sem.at[i]) for i, (src, dst) in enumerate(early + late)
    ]
    early, late = loads[: len(early)], loads[len(early) :]
    k_load = {e: pltpu.make_async_copy(pair_of(keys, e), k_buf.at[e], k_sem.at[e]) for e in order}
    v_load = {e: pltpu.make_async_copy(pair_of(values, e), v_buf.at[e], v_sem.at[e]) for e in order}
    spans = [order[i : i + SPAN] for i in range(0, n_chip, SPAN)]
    for load in early:
        load.start()
    for g, span in enumerate(spans):
        for e in span:
            k_load[e].start()
        for e in spans[g - 1] if g else ():
            v_load[e].start()
    for e in spans[-1]:
        v_load[e].start()
    for load in late:
        load.start()

    barrier = pltpu.get_barrier_semaphore()

    @pl.when(core == PAIR - 1)
    def _():
        for e in order:
            for c in range(PAIR):
                if e or c != PAIR - 1:
                    pl.semaphore_signal(
                        barrier,
                        inc=1,
                        device_id={"seq": chip_at(e) * PAIR + c},
                        device_id_type=MESH,
                    )
        for e in far_first(n_head)[:-1]:
            pl.semaphore_signal(barrier, inc=1, device_id={"head": head_at(e)}, device_id_type=MESH)

    for load in early:
        load.wait()
    row = lax.broadcasted_iota(jnp.int32, (users, LANES), 0)
    limit = jnp.zeros((users, LANES), jnp.int32)
    for u in range(users):
        limit = jnp.where(row == u, len_buf[u], limit)
    lane = lax.broadcasted_iota(jnp.int32, (8, LANES), 1)
    time_table, action_table = lane_table(tbias_buf[...]), lane_table(abias_buf[...])
    for r in range(0, users, 8):
        for c in range(0, block_len, LANES):
            bias = jnp.take_along_axis(
                time_table, tb_buf[r : r + 8, c : c + LANES], axis=1
            ) + jnp.take_along_axis(action_table, ac_buf[r : r + 8, c : c + LANES], axis=1)
            valid = me * block_len + c + lane < limit[r : r + 8]
            bias_buf[r : r + 8, c : c + LANES] = jnp.where(valid, bias * LOG2E, -1e30)

    diag = lax.broadcasted_iota(jnp.int32, (cands, LANES), 1) - lax.broadcasted_iota(
        jnp.int32, (cands, LANES), 0
    )

    def as_row(columns):
        spread = jnp.zeros((cands, LANES), f32)
        for k, column in columns.items():
            spread = jnp.where(diag == k * cands, column, spread)
        return jnp.sum(spread, axis=0, keepdims=True)

    def as_column(line, k):
        picked = jnp.where(diag == k * cands, line, 0.0)
        return jnp.sum(picked, axis=1, keepdims=True)

    def score(g):
        for i, e in enumerate(spans[g]):
            for c in range(PAIR):
                user = chip_at(e) * PAIR + c
                score_buf[g % 2, i, c] = (
                    lax.dot_general(
                        q_buf[user],
                        k_buf[e, c],
                        (((1,), (1,)), ((), ())),
                        preferred_element_type=f32,
                    )
                    * scale
                    + bias_buf[pl.ds(user, 1), :]
                )

    def soften(g):
        parts = {}
        for i, e in enumerate(spans[g]):
            for c in range(PAIR):
                scores = score_buf[g % 2, i, c]
                top = jnp.max(scores, axis=1, keepdims=True)
                weights = jnp.exp2(scores - top)
                parts[e, c] = (
                    top,
                    jnp.sum(weights, axis=1, keepdims=True),
                    weights.astype(bf16),
                )
        return parts

    def message(g, parts, place, e):
        columns = {}
        for c in range(PAIR):
            top, total, weights = parts[e, c]
            place[c * cands : (c + 1) * cands, :] = jnp.dot(
                weights, v_buf[e, c], preferred_element_type=f32
            )
            columns[2 * c], columns[2 * c + 1] = top, total
        place[pair_rows : pair_rows + 1, :] = as_row(columns)

    def to_owner(e):
        return pltpu.make_async_remote_copy(
            src_ref=send1.at[e],
            dst_ref=recv1.at[e, core],
            send_sem=send_sem1.at[e],
            recv_sem=recv_sem1.at[e, core],
            device_id={"seq": chip_at(e) * PAIR + PAIR - 1},
            device_id_type=MESH,
        )

    for e in spans[0]:
        k_load[e].wait()
    score(0)
    for g, span in enumerate(spans):
        for e in spans[g + 1] if g + 1 < len(spans) else ():
            k_load[e].wait()
        for e in span:
            v_load[e].wait()
        if g + 1 < len(spans):
            score(g + 1)
        parts = soften(g)
        for e in span:
            message(g, parts, send1.at[e], e)
        if g == 0:

            @pl.when(core == PAIR - 1)
            def _():
                pl.semaphore_wait(barrier, n_chip - 1 + n_head - 1)

            @pl.when(core != PAIR - 1)
            def _():
                pl.semaphore_wait(barrier, n_chip)

        for e in span:
            if e:
                to_owner(e).start()
    for load in late:
        load.wait()

    back = pltpu.make_async_remote_copy(
        src_ref=send3,
        dst_ref=recv3,
        send_sem=send_sem3,
        recv_sem=recv_sem3,
        device_id={"seq": chip * PAIR},
        device_id_type=MESH,
    )

    @pl.when(core != PAIR - 1)
    def _():
        to_owner(0).start()
        to_owner(0).wait_send()
        back.wait_recv()
        out[0] = recv3[...].astype(out.dtype)

    @pl.when(core == PAIR - 1)
    def _():
        own, own_value, gated = {}, {}, {}
        for c in range(PAIR):
            own_query = q_buf[chip * PAIR + c].astype(f32)
            own[2 * c] = (
                jnp.sum(own_query * nk_buf[c].astype(f32), axis=1, keepdims=True) * scale
            )
            own_value[c] = nv_buf[c].astype(f32)
            gates = gate_buf[c].astype(f32)
            gated[c] = gain_buf[...] * (gates / (1.0 + jnp.exp(-gates)))
        own = as_row(own)

        slots = [(e, c) for e in range(n_chip) for c in range(PAIR)]
        for e, c in slots:
            if e or c != PAIR - 1:
                pltpu.make_async_remote_copy(
                    src_ref=send1.at[e],
                    dst_ref=recv1.at[e, c],
                    send_sem=send_sem1.at[e],
                    recv_sem=recv_sem1.at[e, c],
                    device_id={"seq": chip * PAIR},
                    device_id_type=MESH,
                ).wait_recv()

        def slot(e, c):
            return recv1.at[e, c] if e or c != PAIR - 1 else send1.at[0]

        marks = jnp.zeros((len(slots), LANES), f32)
        place = lax.broadcasted_iota(jnp.int32, marks.shape, 0)
        for s, (e, c) in enumerate(slots):
            marks = jnp.where(place == s, slot(e, c)[pair_rows : pair_rows + 1, :], marks)
        overall = jnp.maximum(jnp.max(marks, axis=0, keepdims=True), own)
        factors = jnp.exp2(marks - overall)
        own_factor = jnp.exp2(own - overall)
        totals = pltpu.roll(marks, LANES - cands, 1)
        denom = own_factor + jnp.sum(factors * totals, axis=0, keepdims=True)
        hidden, squares = [], {}
        for c in range(PAIR):
            numer = as_column(own_factor, 2 * c) * own_value[c]
            for s, (e, k) in enumerate(slots):
                numer = numer + as_column(factors[s : s + 1], 2 * c) * slot(e, k)[
                    c * cands : (c + 1) * cands, :
                ]
            attended = numer / as_column(denom, 2 * c)
            squares[2 * c] = jnp.sum(attended * attended, axis=1, keepdims=True)
            hidden.append((attended * gated[c]).astype(bf16))
        hidden = jnp.concatenate(hidden, axis=0)
        squares = as_row(squares)
        for h in range(n_head):
            send2[h, 0:pair_rows, :] = jnp.dot(
                hidden, w_buf[:, h * width : (h + 1) * width], preferred_element_type=f32
            )
            send2[h, pair_rows : pair_rows + 1, :] = squares
        across = []
        for e in far_first(n_head)[:-1]:
            copy = pltpu.make_async_remote_copy(
                src_ref=send2.at[head_at(e)],
                dst_ref=recv2.at[e],
                send_sem=send_sem2.at[e],
                recv_sem=recv_sem2.at[e],
                device_id={"head": head_at(e)},
                device_id_type=MESH,
            )
            copy.start()
            across.append(copy)
        whole = send2[my_head]
        for copy in across:
            copy.wait_recv()
        for e in range(1, n_head):
            whole = whole + recv2[e]
        line = whole[pair_rows : pair_rows + 1]
        final = []
        for c in range(PAIR):
            square_sum = as_column(line, 2 * c)
            factor = 1.0 / jnp.sqrt(square_sum / (width * n_head) + 1e-06)
            final.append(whole[c * cands : (c + 1) * cands] * factor)
        send3[...] = final[0]
        back.start()
        out[0] = final[1].astype(out.dtype)
        for copy in across:
            copy.wait_send()
        back.wait_send()

    for e in order[:-1]:
        to_owner(e).wait_send()


def body(
    query,
    new_key,
    new_value,
    keys,
    values,
    lengths,
    time_bucket,
    action,
    time_bias,
    action_bias,
    gate,
    norm_gain,
    w_out,
):
    users, block_len, width = keys.shape
    cands = query.shape[1]
    n_seq, n_head = lax.axis_size("seq"), lax.axis_size("head")
    assert users == n_seq and width == LANES and w_out.shape[1] == n_head * width
    assert n_seq % (PAIR * SPAN) == 0 and 4 * cands <= LANES
    n_chip = n_seq // PAIR
    tile = PAIR * cands + 1
    bf16, f32, i32 = jnp.bfloat16, jnp.float32, jnp.int32
    vmem, dma = pltpu.VMEM, pltpu.SemaphoreType.DMA
    buckets, actions = time_bias.shape[0], action_bias.shape[0]
    return pl.pallas_call(
        kernel,
        name="decode",
        out_shape=jax.ShapeDtypeStruct((users // n_seq, cands, width), bf16),
        in_specs=[pl.BlockSpec(memory_space=pl.ANY)] * 13,
        out_specs=pl.BlockSpec(memory_space=vmem),
        scratch_shapes=[
            vmem((users, cands, width), bf16),
            vmem((PAIR, cands, width), bf16),
            vmem((PAIR, cands, width), bf16),
            vmem((n_chip, PAIR, block_len, width), bf16),
            vmem((n_chip, PAIR, block_len, width), bf16),
            pltpu.SMEM((users,), i32),
            vmem((users, block_len), i32),
            vmem((users, block_len), i32),
            vmem((1, buckets), f32),
            vmem((1, actions), f32),
            vmem((PAIR, cands, width), bf16),
            vmem((1, width), f32),
            vmem((width, n_head * width), bf16),
            vmem((users, block_len), f32),
            vmem((2, SPAN, PAIR, cands, block_len), f32),
            vmem((n_chip, tile, width), f32),
            vmem((n_chip, PAIR, tile, width), f32),
            vmem((n_head, tile, width), f32),
            vmem((n_head, tile, width), f32),
            vmem((cands, width), f32),
            vmem((cands, width), f32),
            dma((11,)),
            dma((n_chip,)),
            dma((n_chip,)),
            dma((n_chip,)),
            dma((n_chip, PAIR)),
            dma((n_head,)),
            dma((n_head,)),
            dma,
            dma,
        ],
        compiler_params=pltpu.CompilerParams(collective_id=0, has_side_effects=True),
    )(
        query,
        new_key,
        new_value,
        keys,
        values,
        lengths,
        time_bucket,
        action,
        time_bias.reshape(1, buckets),
        action_bias.reshape(1, actions),
        gate,
        norm_gain.reshape(1, width),
        w_out,
    )


def solution(mesh):
    placed = (
        P("groups", None, "head"),
        P("groups", None, "head"),
        P("groups", None, "head"),
        P("groups", "seq", "head"),
        P("groups", "seq", "head"),
        P("groups"),
        P("groups", "seq"),
        P("groups", "seq"),
        P(None, "head"),
        P(None, "head"),
        P("groups", None, "head"),
        P("head"),
        P("head", None),
    )
    return jax.shard_map(
        body,
        mesh=mesh,
        in_specs=placed,
        out_specs=P(("groups", "seq"), None, "head"),
        check_vma=False,
    )
```

```python
import math

import jax
import jax.numpy as jnp
from jax import lax
from jax.experimental import pallas as pl
from jax.experimental.pallas import tpu as pltpu
from jax.sharding import PartitionSpec as P

MESH = pl.DeviceIdType.MESH
LOG2E = math.log2(math.e)
LANES = 128
PAIR = 2
SPAN = 2


def far_first(count):
    return sorted(range(count), key=lambda d: (-min(d, count - d), d))


def lane_table(table):
    rows = jnp.broadcast_to(table, (8, table.shape[1]))
    rest = LANES - table.shape[1]
    if rest:
        rows = jnp.concatenate([rows, jnp.zeros((8, rest), rows.dtype)], axis=1)
    return rows


def kernel(
    query,
    new_key,
    new_value,
    keys,
    values,
    lengths,
    time_bucket,
    action,
    time_bias,
    action_bias,
    gate,
    norm_gain,
    w_out,
    out,
    q_buf,
    nk_buf,
    nv_buf,
    k_buf,
    v_buf,
    len_buf,
    tb_buf,
    ac_buf,
    tbias_buf,
    abias_buf,
    gate_buf,
    gain_buf,
    w_buf,
    bias_buf,
    score_buf,
    send1,
    recv1,
    send2,
    recv2,
    send3,
    recv3,
    in_sem,
    k_sem,
    v_sem,
    send_sem1,
    recv_sem1,
    send_sem2,
    recv_sem2,
    send_sem3,
    recv_sem3,
):
    n_seq = lax.axis_size("seq")
    n_head = lax.axis_size("head")
    n_chip = n_seq // PAIR
    me = lax.axis_index("seq")
    chip, core = lax.div(me, PAIR), lax.rem(me, PAIR)
    my_head = lax.axis_index("head")
    users, cands, width = query.shape
    block_len = keys.shape[1]
    pair_rows = PAIR * cands
    scale = LOG2E / math.sqrt(width)
    order = [0, 1] + [e for e in far_first(n_chip) if e > 1]
    f32, bf16 = jnp.float32, jnp.bfloat16

    def chip_at(e):
        return lax.rem(chip + e, n_chip)

    def head_at(e):
        return lax.rem(my_head + e, n_head)

    def pair_of(source, e):
        return source.at[pl.ds(chip_at(e) * PAIR, PAIR)]

    early = [
        (query, q_buf),
        (lengths, len_buf),
        (time_bias, tbias_buf),
        (action_bias, abias_buf),
        (time_bucket, tb_buf),
        (action, ac_buf),
    ]
    late = [
        (pair_of(new_key, 0), nk_buf),
        (pair_of(new_value, 0), nv_buf),
        (pair_of(gate, 0), gate_buf),
        (norm_gain, gain_buf),
        (w_out, w_buf),
    ]
    loads = [
        pltpu.make_async_copy(src, dst, in_sem.at[i]) for i, (src, dst) in enumerate(early + late)
    ]
    early, late = loads[: len(early)], loads[len(early) :]
    k_load = {e: pltpu.make_async_copy(pair_of(keys, e), k_buf.at[e], k_sem.at[e]) for e in order}
    v_load = {e: pltpu.make_async_copy(pair_of(values, e), v_buf.at[e], v_sem.at[e]) for e in order}
    spans = [order[i : i + SPAN] for i in range(0, n_chip, SPAN)]
    early[0].start()
    for e in spans[0]:
        k_load[e].start()
    for load in early[1:]:
        load.start()
    for g, span in enumerate(spans):
        for e in span if g else ():
            k_load[e].start()
        for e in spans[g - 1] if g else ():
            v_load[e].start()
    for e in spans[-1]:
        v_load[e].start()
    for load in late:
        load.start()

    barrier = pltpu.get_barrier_semaphore()

    @pl.when(core == PAIR - 1)
    def _():
        for e in far_first(n_chip):
            for c in range(PAIR):
                if e or c != PAIR - 1:
                    pl.semaphore_signal(
                        barrier,
                        inc=1,
                        device_id={"seq": chip_at(e) * PAIR + c},
                        device_id_type=MESH,
                    )
        for e in far_first(n_head)[:-1]:
            pl.semaphore_signal(barrier, inc=1, device_id={"head": head_at(e)}, device_id_type=MESH)

    diag = lax.broadcasted_iota(jnp.int32, (cands, LANES), 1) - lax.broadcasted_iota(
        jnp.int32, (cands, LANES), 0
    )

    def as_row(columns):
        spread = jnp.zeros((cands, LANES), f32)
        for k, column in columns.items():
            spread = jnp.where(diag == k * cands, column, spread)
        return jnp.sum(spread, axis=0, keepdims=True)

    def as_column(line, k):
        picked = jnp.where(diag == k * cands, line, 0.0)
        return jnp.sum(picked, axis=1, keepdims=True)

    def score(g):
        for e in spans[g]:
            for c in range(PAIR):
                score_buf[e, c] = lax.dot_general(
                    q_buf[chip_at(e) * PAIR + c],
                    k_buf[e, c],
                    (((1,), (1,)), ((), ())),
                    preferred_element_type=f32,
                )

    def soften(g):
        parts = {}
        for e in spans[g]:
            columns = {}
            for c in range(PAIR):
                user = chip_at(e) * PAIR + c
                scores = score_buf[e, c] * scale + bias_buf[pl.ds(user, 1), :]
                top = jnp.max(scores, axis=1, keepdims=True)
                weights = jnp.exp2(scores - top)
                parts[e, c] = weights.astype(bf16)
                columns[2 * c] = top
                columns[2 * c + 1] = jnp.sum(weights, axis=1, keepdims=True)
            send1[e, pair_rows : pair_rows + 1, :] = as_row(columns)
        return parts

    def weigh(parts, e):
        for c in range(PAIR):
            send1[e, c * cands : (c + 1) * cands, :] = jnp.dot(
                parts[e, c], v_buf[e, c], preferred_element_type=f32
            )

    def to_owner(e):
        return pltpu.make_async_remote_copy(
            src_ref=send1.at[e],
            dst_ref=recv1.at[e, core],
            send_sem=send_sem1.at[e],
            recv_sem=recv_sem1.at[e, core],
            device_id={"seq": chip_at(e) * PAIR + PAIR - 1},
            device_id_type=MESH,
        )

    early[0].wait()
    for e in spans[0]:
        k_load[e].wait()
    score(0)

    for load in early[1:]:
        load.wait()
    row = lax.broadcasted_iota(jnp.int32, (users, LANES), 0)
    limit = jnp.zeros((users, LANES), jnp.int32)
    for u in range(users):
        limit = jnp.where(row == u, len_buf[u], limit)
    lane = lax.broadcasted_iota(jnp.int32, (8, LANES), 1)
    time_table, action_table = lane_table(tbias_buf[...]), lane_table(abias_buf[...])
    for r in range(0, users, 8):
        for c in range(0, block_len, LANES):
            bias = jnp.take_along_axis(
                time_table, tb_buf[r : r + 8, c : c + LANES], axis=1
            ) + jnp.take_along_axis(action_table, ac_buf[r : r + 8, c : c + LANES], axis=1)
            valid = me * block_len + c + lane < limit[r : r + 8]
            bias_buf[r : r + 8, c : c + LANES] = jnp.where(valid, bias * LOG2E, -1e30)

    for g, span in enumerate(spans):
        if g + 1 < len(spans):
            for e in spans[g + 1]:
                k_load[e].wait()
            for e in span:
                v_load[e].wait()
            score(g + 1)
            parts = soften(g)
        else:
            parts = soften(g)
            for e in span:
                v_load[e].wait()
        for e in span:
            weigh(parts, e)

        @pl.when(core != PAIR - 1)
        def _():
            if g == 0:
                pl.semaphore_wait(barrier, n_chip)
            for e in span:
                to_owner(e).start()

    @pl.when(core == PAIR - 1)
    def _():
        pl.semaphore_wait(barrier, n_chip - 1 + n_head - 1)
        for e in far_first(n_chip)[:-1]:
            to_owner(e).start()

    for load in late:
        load.wait()

    back = pltpu.make_async_remote_copy(
        src_ref=send3,
        dst_ref=recv3,
        send_sem=send_sem3,
        recv_sem=recv_sem3,
        device_id={"seq": chip * PAIR},
        device_id_type=MESH,
    )

    @pl.when(core != PAIR - 1)
    def _():
        back.wait_recv()
        out[0] = recv3[...].astype(out.dtype)
        to_owner(0).wait_send()

    @pl.when(core == PAIR - 1)
    def _():
        own, own_value, gated = {}, {}, {}
        for c in range(PAIR):
            own_query = q_buf[chip * PAIR + c].astype(f32)
            own[2 * c] = (
                jnp.sum(own_query * nk_buf[c].astype(f32), axis=1, keepdims=True) * scale
            )
            own_value[c] = nv_buf[c].astype(f32)
            gates = gate_buf[c].astype(f32)
            gated[c] = gain_buf[...] * (gates / (1.0 + jnp.exp(-gates)))
        own = as_row(own)

        slots = [(e, c) for e in range(n_chip) for c in range(PAIR)]
        for e, c in slots:
            if e or c != PAIR - 1:
                pltpu.make_async_remote_copy(
                    src_ref=send1.at[e],
                    dst_ref=recv1.at[e, c],
                    send_sem=send_sem1.at[e],
                    recv_sem=recv_sem1.at[e, c],
                    device_id={"seq": chip * PAIR},
                    device_id_type=MESH,
                ).wait_recv()

        def slot(e, c):
            return recv1.at[e, c] if e or c != PAIR - 1 else send1.at[0]

        marks = jnp.zeros((len(slots), LANES), f32)
        place = lax.broadcasted_iota(jnp.int32, marks.shape, 0)
        for s, (e, c) in enumerate(slots):
            marks = jnp.where(place == s, slot(e, c)[pair_rows : pair_rows + 1, :], marks)
        overall = jnp.maximum(jnp.max(marks, axis=0, keepdims=True), own)
        factors = jnp.exp2(marks - overall)
        own_factor = jnp.exp2(own - overall)
        totals = pltpu.roll(marks, LANES - cands, 1)
        denom = own_factor + jnp.sum(factors * totals, axis=0, keepdims=True)
        hidden, squares = [], {}
        for c in range(PAIR):
            numer = as_column(own_factor, 2 * c) * own_value[c]
            for s, (e, k) in enumerate(slots):
                numer = numer + as_column(factors[s : s + 1], 2 * c) * slot(e, k)[
                    c * cands : (c + 1) * cands, :
                ]
            attended = numer / as_column(denom, 2 * c)
            squares[2 * c] = jnp.sum(attended * attended, axis=1, keepdims=True)
            hidden.append((attended * gated[c]).astype(bf16))
        hidden = jnp.concatenate(hidden, axis=0)
        squares = as_row(squares)
        for h in range(n_head):
            send2[h, 0:pair_rows, :] = jnp.dot(
                hidden, w_buf[:, h * width : (h + 1) * width], preferred_element_type=f32
            )
            send2[h, pair_rows : pair_rows + 1, :] = squares
        across = []
        for e in far_first(n_head)[:-1]:
            copy = pltpu.make_async_remote_copy(
                src_ref=send2.at[head_at(e)],
                dst_ref=recv2.at[e],
                send_sem=send_sem2.at[e],
                recv_sem=recv_sem2.at[e],
                device_id={"head": head_at(e)},
                device_id_type=MESH,
            )
            copy.start()
            across.append(copy)
        whole = send2[my_head]
        for copy in across:
            copy.wait_recv()
        for e in range(1, n_head):
            whole = whole + recv2[e]
        line = whole[pair_rows : pair_rows + 1]
        final = []
        for c in range(PAIR):
            square_sum = as_column(line, 2 * c)
            factor = 1.0 / jnp.sqrt(square_sum / (width * n_head) + 1e-06)
            final.append(whole[c * cands : (c + 1) * cands] * factor)
        send3[...] = final[0]
        back.start()
        out[0] = final[1].astype(out.dtype)
        for copy in across:
            copy.wait_send()
        back.wait_send()

    for e in order[1:]:
        to_owner(e).wait_send()


def body(
    query,
    new_key,
    new_value,
    keys,
    values,
    lengths,
    time_bucket,
    action,
    time_bias,
    action_bias,
    gate,
    norm_gain,
    w_out,
):
    users, block_len, width = keys.shape
    cands = query.shape[1]
    n_seq, n_head = lax.axis_size("seq"), lax.axis_size("head")
    assert users == n_seq and width == LANES and w_out.shape[1] == n_head * width
    assert n_seq % (PAIR * SPAN) == 0 and 4 * cands <= LANES
    n_chip = n_seq // PAIR
    tile = PAIR * cands + 1
    bf16, f32, i32 = jnp.bfloat16, jnp.float32, jnp.int32
    vmem, dma = pltpu.VMEM, pltpu.SemaphoreType.DMA
    buckets, actions = time_bias.shape[0], action_bias.shape[0]
    return pl.pallas_call(
        kernel,
        name="decode",
        out_shape=pltpu.VMEM((users // n_seq, cands, width), bf16),
        in_specs=[pl.BlockSpec(memory_space=pl.ANY)] * 13,
        out_specs=pl.BlockSpec(memory_space=vmem),
        scratch_shapes=[
            vmem((users, cands, width), bf16),
            vmem((PAIR, cands, width), bf16),
            vmem((PAIR, cands, width), bf16),
            vmem((n_chip, PAIR, block_len, width), bf16),
            vmem((n_chip, PAIR, block_len, width), bf16),
            pltpu.SMEM((users,), i32),
            vmem((users, block_len), i32),
            vmem((users, block_len), i32),
            vmem((1, buckets), f32),
            vmem((1, actions), f32),
            vmem((PAIR, cands, width), bf16),
            vmem((1, width), f32),
            vmem((width, n_head * width), bf16),
            vmem((users, block_len), f32),
            vmem((n_chip, PAIR, cands, block_len), f32),
            vmem((n_chip, tile, width), f32),
            vmem((n_chip, PAIR, tile, width), f32),
            vmem((n_head, tile, width), f32),
            vmem((n_head, tile, width), f32),
            vmem((cands, width), f32),
            vmem((cands, width), f32),
            dma((11,)),
            dma((n_chip,)),
            dma((n_chip,)),
            dma((n_chip,)),
            dma((n_chip, PAIR)),
            dma((n_head,)),
            dma((n_head,)),
            dma,
            dma,
        ],
        compiler_params=pltpu.CompilerParams(collective_id=0, has_side_effects=True),
    )(
        query,
        new_key,
        new_value,
        keys,
        values,
        lengths,
        time_bucket,
        action,
        time_bias.reshape(1, buckets),
        action_bias.reshape(1, actions),
        gate,
        norm_gain.reshape(1, width),
        w_out,
    )


def solution(mesh):
    placed = (
        P("groups", None, "head"),
        P("groups", None, "head"),
        P("groups", None, "head"),
        P("groups", "seq", "head"),
        P("groups", "seq", "head"),
        P("groups"),
        P("groups", "seq"),
        P("groups", "seq"),
        P(None, "head"),
        P(None, "head"),
        P("groups", None, "head"),
        P("head"),
        P("head", None),
    )
    return jax.shard_map(
        body,
        mesh=mesh,
        in_specs=placed,
        out_specs=P(("groups", "seq"), None, "head"),
        check_vma=False,
    )
```

```python
import math

import jax
import jax.numpy as jnp
from jax import lax
from jax.experimental import pallas as pl
from jax.experimental.pallas import tpu as pltpu
from jax.sharding import PartitionSpec as P

MESH = pl.DeviceIdType.MESH
LOG2E = math.log2(math.e)
LANES = 128
PAIR = 2
SPAN = 2


def far_first(count):
    return sorted(range(count), key=lambda d: (-min(d, count - d), d))


def lane_table(table):
    rows = jnp.broadcast_to(table, (8, table.shape[1]))
    rest = LANES - table.shape[1]
    if rest:
        rows = jnp.concatenate([rows, jnp.zeros((8, rest), rows.dtype)], axis=1)
    return rows


def kernel(
    query,
    new_key,
    new_value,
    keys,
    values,
    lengths,
    time_bucket,
    action,
    time_bias,
    action_bias,
    gate,
    norm_gain,
    w_out,
    out,
    q_buf,
    nk_buf,
    nv_buf,
    k_buf,
    v_buf,
    len_buf,
    tb_buf,
    ac_buf,
    tbias_buf,
    abias_buf,
    gate_buf,
    gain_buf,
    w_buf,
    bias_buf,
    score_buf,
    send1,
    recv1,
    send2,
    recv2,
    in_sem,
    k_sem,
    v_sem,
    send_sem1,
    recv_sem1,
    send_sem2,
    recv_sem2,
    ring_sem,
):
    n_seq = lax.axis_size("seq")
    n_head = lax.axis_size("head")
    n_chip = n_seq // PAIR
    me = lax.axis_index("seq")
    chip, core = lax.div(me, PAIR), lax.rem(me, PAIR)
    my_head = lax.axis_index("head")
    users, cands, width = query.shape
    block_len = keys.shape[1]
    pair_rows = PAIR * cands
    scale = LOG2E / math.sqrt(width)
    far = far_first(n_chip)[:-1]
    order = [0, far[0], 1] + [e for e in far[1:] if e != 1]
    f32, bf16 = jnp.float32, jnp.bfloat16

    def chip_at(e):
        return lax.rem(chip + e, n_chip)

    def head_at(e):
        return lax.rem(my_head + e, n_head)

    def pair_of(source, e):
        return source.at[pl.ds(chip_at(e) * PAIR, PAIR)]

    early = [
        (query, q_buf),
        (lengths, len_buf),
        (time_bias, tbias_buf),
        (action_bias, abias_buf),
        (time_bucket, tb_buf),
        (action, ac_buf),
    ]
    late = [
        (pair_of(new_key, 0), nk_buf),
        (pair_of(new_value, 0), nv_buf),
        (pair_of(gate, 0), gate_buf),
        (norm_gain, gain_buf),
        (w_out, w_buf),
    ]
    loads = [
        pltpu.make_async_copy(src, dst, in_sem.at[i]) for i, (src, dst) in enumerate(early + late)
    ]
    early, late = loads[: len(early)], loads[len(early) :]
    spans = [order[i : i + SPAN] for i in range(0, n_chip, SPAN)]

    def start_span(source, buf, sem, g):
        for i, e in enumerate(spans[g]):
            pltpu.make_async_copy(
                pair_of(source, e), buf.at[g, pl.ds(i * PAIR, PAIR)], sem.at[g]
            ).start()

    def wait_span(source, buf, sem, g):
        pltpu.make_async_copy(source.at[pl.ds(0, SPAN * PAIR)], buf.at[g], sem.at[g]).wait()

    early[0].start()
    start_span(keys, k_buf, k_sem, 0)
    for load in early[1:]:
        load.start()
    for g in range(1, len(spans)):
        start_span(keys, k_buf, k_sem, g)
        start_span(values, v_buf, v_sem, g - 1)
    start_span(values, v_buf, v_sem, len(spans) - 1)
    for load in late:
        load.start()

    barrier = pltpu.get_barrier_semaphore()

    @pl.when(core == PAIR - 1)
    def _():
        for e in far + [0]:
            pl.semaphore_signal(
                barrier, inc=1, device_id={"seq": chip_at(e) * PAIR}, device_id_type=MESH
            )

    for e in far_first(n_head)[:-1]:
        pl.semaphore_signal(
            barrier,
            inc=1,
            device_id={"seq": chip * PAIR + PAIR - 1, "head": head_at(e)},
            device_id_type=MESH,
        )

    diag = lax.broadcasted_iota(jnp.int32, (cands, LANES), 1) - lax.broadcasted_iota(
        jnp.int32, (cands, LANES), 0
    )

    def as_row(columns):
        spread = jnp.zeros((cands, LANES), f32)
        for k, column in columns.items():
            spread = jnp.where(diag == k * cands, column, spread)
        return jnp.sum(spread, axis=0, keepdims=True)

    def as_column(line, k):
        picked = jnp.where(diag == k * cands, line, 0.0)
        return jnp.sum(picked, axis=1, keepdims=True)

    def score(g):
        for i, e in enumerate(spans[g]):
            for c in range(PAIR):
                score_buf[e, c] = lax.dot_general(
                    q_buf[chip_at(e) * PAIR + c],
                    k_buf[g, i * PAIR + c],
                    (((1,), (1,)), ((), ())),
                    preferred_element_type=f32,
                )

    def soften(g):
        parts = {}
        for e in spans[g]:
            columns = {}
            for c in range(PAIR):
                user = chip_at(e) * PAIR + c
                scores = score_buf[e, c] * scale + bias_buf[pl.ds(user, 1), :]
                top = jnp.max(scores, axis=1, keepdims=True)
                weights = jnp.exp2(scores - top)
                parts[e, c] = weights.astype(bf16)
                columns[2 * c] = top
                columns[2 * c + 1] = jnp.sum(weights, axis=1, keepdims=True)
            send1[e, pair_rows : pair_rows + 1, :] = as_row(columns)
        return parts

    def weigh(g, parts):
        for i, e in enumerate(spans[g]):
            for c in range(PAIR):
                send1[e, c * cands : (c + 1) * cands, :] = jnp.dot(
                    parts[e, c], v_buf[g, i * PAIR + c], preferred_element_type=f32
                )

    def to_owner(e):
        return pltpu.make_async_remote_copy(
            src_ref=send1.at[e],
            dst_ref=recv1.at[e * PAIR - 1 + core if e else 0],
            send_sem=send_sem1,
            recv_sem=recv_sem1,
            device_id={"seq": chip_at(e) * PAIR + PAIR - 1},
            device_id_type=MESH,
        )

    early[0].wait()
    wait_span(keys, k_buf, k_sem, 0)
    score(0)

    for load in early[1:]:
        load.wait()
    row = lax.broadcasted_iota(jnp.int32, (users, LANES), 0)
    limit = jnp.zeros((users, LANES), jnp.int32)
    for u in range(users):
        limit = jnp.where(row == u, len_buf[u], limit)
    lane = lax.broadcasted_iota(jnp.int32, (8, LANES), 1)
    time_table, action_table = lane_table(tbias_buf[...]), lane_table(abias_buf[...])
    for r in range(0, users, 8):
        for c in range(0, block_len, LANES):
            bias = jnp.take_along_axis(
                time_table, tb_buf[r : r + 8, c : c + LANES], axis=1
            ) + jnp.take_along_axis(action_table, ac_buf[r : r + 8, c : c + LANES], axis=1)
            valid = me * block_len + c + lane < limit[r : r + 8]
            bias_buf[r : r + 8, c : c + LANES] = jnp.where(valid, bias * LOG2E, -1e30)

    ready = len(spans) - 2
    for g, span in enumerate(spans):
        if g + 1 < len(spans):
            wait_span(keys, k_buf, k_sem, g + 1)
            wait_span(values, v_buf, v_sem, g)
            score(g + 1)
            parts = soften(g)
        else:
            parts = soften(g)
            wait_span(values, v_buf, v_sem, g)
        weigh(g, parts)

        @pl.when(core != PAIR - 1)
        def _():
            if g == 0:
                pl.semaphore_wait(barrier, n_chip)
                pl.semaphore_signal(
                    ring_sem, inc=1, device_id={"seq": me + 1}, device_id_type=MESH
                )
            for e in span:
                to_owner(e).start()

        if g >= ready:

            @pl.when(core == PAIR - 1)
            def _():
                if g == ready:
                    pl.semaphore_wait(ring_sem, 1)
                done = order[: (ready + 1) * SPAN] if g == ready else span
                for e in far:
                    if e in done:
                        to_owner(e).start()

    for load in late:
        load.wait()

    def across(e, c):
        return pltpu.make_async_remote_copy(
            src_ref=send2.at[head_at(e) * PAIR + c],
            dst_ref=recv2.at[e],
            send_sem=send_sem2,
            recv_sem=recv_sem2,
            device_id={"seq": chip * PAIR + c, "head": head_at(e)},
            device_id_type=MESH,
        )

    def arrived(buf, sem):
        pltpu.make_async_remote_copy(
            src_ref=buf,
            dst_ref=buf,
            send_sem=send_sem2,
            recv_sem=sem,
            device_id={"seq": chip * PAIR + PAIR - 1 - core},
            device_id_type=MESH,
        ).wait_recv()

    def gone(buf, sem):
        pltpu.make_async_remote_copy(
            src_ref=buf,
            dst_ref=buf,
            send_sem=sem,
            recv_sem=recv_sem2,
            device_id={"seq": chip * PAIR + PAIR - 1 - core},
            device_id_type=MESH,
        ).wait_send()

    def finish():
        whole = recv2[0]
        for e in range(1, n_head):
            whole = whole + recv2[e]
        square_sum = as_column(whole[cands : cands + 1], 0)
        factor = 1.0 / jnp.sqrt(square_sum / (width * n_head) + 1e-06)
        out[0] = (whole[:cands] * factor).astype(out.dtype)

    @pl.when(core != PAIR - 1)
    def _():
        arrived(recv2, recv_sem2)
        finish()
        gone(send1, send_sem1)

    @pl.when(core == PAIR - 1)
    def _():
        own, own_value, gated = {}, {}, {}
        for c in range(PAIR):
            own_query = q_buf[chip * PAIR + c].astype(f32)
            own[2 * c] = (
                jnp.sum(own_query * nk_buf[c].astype(f32), axis=1, keepdims=True) * scale
            )
            own_value[c] = nv_buf[c].astype(f32)
            gates = gate_buf[c].astype(f32)
            gated[c] = gain_buf[...] * (gates / (1.0 + jnp.exp(-gates)))
        own = as_row(own)
        arrived(recv1, recv_sem1)

        slots = [recv1.at[i] for i in range(n_seq - 1)] + [send1.at[0]]
        marks = jnp.zeros((n_seq, LANES), f32)
        place = lax.broadcasted_iota(jnp.int32, marks.shape, 0)
        for i, slot in enumerate(slots):
            marks = jnp.where(place == i, slot[pair_rows : pair_rows + 1, :], marks)
        overall = jnp.maximum(jnp.max(marks, axis=0, keepdims=True), own)
        factors = jnp.exp2(marks - overall)
        own_factor = jnp.exp2(own - overall)
        totals = pltpu.roll(marks, LANES - cands, 1)
        denom = own_factor + jnp.sum(factors * totals, axis=0, keepdims=True)
        hidden, squares = [], {}
        for c in range(PAIR):
            numer = as_column(own_factor, 2 * c) * own_value[c]
            for i, slot in enumerate(slots):
                numer = numer + as_column(factors[i : i + 1], 2 * c) * slot[
                    c * cands : (c + 1) * cands, :
                ]
            attended = numer / as_column(denom, 2 * c)
            squares[c] = as_row({0: jnp.sum(attended * attended, axis=1, keepdims=True)})
            hidden.append((attended * gated[c]).astype(bf16))
        hidden = jnp.concatenate(hidden, axis=0)
        for h in range(n_head):
            part = jnp.dot(
                hidden, w_buf[:, h * width : (h + 1) * width], preferred_element_type=f32
            )
            for c in range(PAIR):
                send2[h * PAIR + c, 0:cands, :] = part[c * cands : (c + 1) * cands]
                send2[h * PAIR + c, cands : cands + 1, :] = squares[c]
        pl.semaphore_wait(barrier, PAIR * (n_head - 1))
        for e in far_first(n_head)[:-1]:
            for c in range(PAIR):
                across(e, c).start()
        across(0, 0).start()
        recv2[0] = send2[my_head * PAIR + PAIR - 1]
        arrived(recv2.at[pl.ds(1, n_head - 1)], recv_sem2)
        finish()
        gone(send1.at[pl.ds(1, n_chip - 1)], send_sem1)
        gone(send2.at[pl.ds(0, n_head * PAIR - 1)], send_sem2)


def body(
    query,
    new_key,
    new_value,
    keys,
    values,
    lengths,
    time_bucket,
    action,
    time_bias,
    action_bias,
    gate,
    norm_gain,
    w_out,
):
    users, block_len, width = keys.shape
    cands = query.shape[1]
    n_seq, n_head = lax.axis_size("seq"), lax.axis_size("head")
    assert users == n_seq and width == LANES and w_out.shape[1] == n_head * width
    assert n_seq % (PAIR * SPAN) == 0 and 4 * cands <= LANES
    n_chip = n_seq // PAIR
    tile = PAIR * cands + 1
    bf16, f32, i32 = jnp.bfloat16, jnp.float32, jnp.int32
    vmem, dma = pltpu.VMEM, pltpu.SemaphoreType.DMA
    buckets, actions = time_bias.shape[0], action_bias.shape[0]
    return pl.pallas_call(
        kernel,
        name="decode",
        out_shape=pltpu.VMEM((users // n_seq, cands, width), bf16),
        in_specs=[pl.BlockSpec(memory_space=pl.ANY)] * 13,
        out_specs=pl.BlockSpec(memory_space=vmem),
        scratch_shapes=[
            vmem((users, cands, width), bf16),
            vmem((PAIR, cands, width), bf16),
            vmem((PAIR, cands, width), bf16),
            vmem((n_chip // SPAN, SPAN * PAIR, block_len, width), bf16),
            vmem((n_chip // SPAN, SPAN * PAIR, block_len, width), bf16),
            pltpu.SMEM((users,), i32),
            vmem((users, block_len), i32),
            vmem((users, block_len), i32),
            vmem((1, buckets), f32),
            vmem((1, actions), f32),
            vmem((PAIR, cands, width), bf16),
            vmem((1, width), f32),
            vmem((width, n_head * width), bf16),
            vmem((users, block_len), f32),
            vmem((n_chip, PAIR, cands, block_len), f32),
            vmem((n_chip, tile, width), f32),
            vmem((n_seq - 1, tile, width), f32),
            vmem((n_head * PAIR, cands + 1, width), f32),
            vmem((n_head, cands + 1, width), f32),
            dma((11,)),
            dma((n_chip // SPAN,)),
            dma((n_chip // SPAN,)),
            dma,
            dma,
            dma,
            dma,
            pltpu.SemaphoreType.REGULAR,
        ],
        compiler_params=pltpu.CompilerParams(collective_id=0, has_side_effects=True),
    )(
        query,
        new_key,
        new_value,
        keys,
        values,
        lengths,
        time_bucket,
        action,
        time_bias.reshape(1, buckets),
        action_bias.reshape(1, actions),
        gate,
        norm_gain.reshape(1, width),
        w_out,
    )


def solution(mesh):
    placed = (
        P("groups", None, "head"),
        P("groups", None, "head"),
        P("groups", None, "head"),
        P("groups", "seq", "head"),
        P("groups", "seq", "head"),
        P("groups"),
        P("groups", "seq"),
        P("groups", "seq"),
        P(None, "head"),
        P(None, "head"),
        P("groups", None, "head"),
        P("head"),
        P("head", None),
    )
    return jax.shard_map(
        body,
        mesh=mesh,
        in_specs=placed,
        out_specs=P(("groups", "seq"), None, "head"),
        check_vma=False,
    )
```

```python
import math

import jax
import jax.numpy as jnp
from jax import lax
from jax.experimental import pallas as pl
from jax.experimental.pallas import tpu as pltpu
from jax.sharding import PartitionSpec as P

MESH = pl.DeviceIdType.MESH
LOG2E = math.log2(math.e)
LANES = 128
PAIR = 2
SPAN = 2


def far_first(count):
    return sorted(range(count), key=lambda d: (-min(d, count - d), d))


def lane_table(table):
    rows = jnp.broadcast_to(table, (8, table.shape[1]))
    rest = LANES - table.shape[1]
    if rest:
        rows = jnp.concatenate([rows, jnp.zeros((8, rest), rows.dtype)], axis=1)
    return rows


def kernel(
    query,
    new_key,
    new_value,
    keys,
    values,
    lengths,
    time_bucket,
    action,
    time_bias,
    action_bias,
    gate,
    norm_gain,
    w_out,
    out,
    q_buf,
    nk_buf,
    nv_buf,
    k_buf,
    v_buf,
    len_buf,
    tb_buf,
    ac_buf,
    tbias_buf,
    abias_buf,
    gate_buf,
    gain_buf,
    w_buf,
    bias_buf,
    score_buf,
    send1,
    recv1,
    send2,
    recv2,
    in_sem,
    k_sem,
    v_sem,
    send_sem1,
    recv_sem1,
    send_sem2,
    recv_sem2,
    told,
):
    n_seq = lax.axis_size("seq")
    n_head = lax.axis_size("head")
    n_chip = n_seq // PAIR
    me = lax.axis_index("seq")
    chip, core = lax.div(me, PAIR), lax.rem(me, PAIR)
    my_head = lax.axis_index("head")
    users, cands, width = query.shape
    block_len = keys.shape[1]
    pair_rows = PAIR * cands
    scale = LOG2E / math.sqrt(width)
    far = far_first(n_chip)[:-1]
    order = [0, far[0], 1] + [e for e in far[1:] if e != 1]
    f32, bf16 = jnp.float32, jnp.bfloat16

    def chip_at(e):
        return lax.rem(chip + e, n_chip)

    def head_at(e):
        return lax.rem(my_head + e, n_head)

    def pair_of(source, e):
        return source.at[pl.ds(chip_at(e) * PAIR, PAIR)]

    early = [
        (query, q_buf),
        (lengths, len_buf),
        (time_bias, tbias_buf),
        (action_bias, abias_buf),
        (time_bucket, tb_buf),
        (action, ac_buf),
    ]
    late = [
        (pair_of(new_key, 0), nk_buf),
        (pair_of(new_value, 0), nv_buf),
        (pair_of(gate, 0), gate_buf),
        (norm_gain, gain_buf),
        (w_out, w_buf),
    ]
    loads = [
        pltpu.make_async_copy(src, dst, in_sem.at[i]) for i, (src, dst) in enumerate(early + late)
    ]
    early, late = loads[: len(early)], loads[len(early) :]
    spans = [order[i : i + SPAN] for i in range(0, n_chip, SPAN)]

    def start_span(source, buf, sem, g):
        for i, e in enumerate(spans[g]):
            pltpu.make_async_copy(
                pair_of(source, e), buf.at[g, pl.ds(i * PAIR, PAIR)], sem.at[g]
            ).start()

    def wait_span(source, buf, sem, g):
        pltpu.make_async_copy(source.at[pl.ds(0, SPAN * PAIR)], buf.at[g], sem.at[g]).wait()

    early[0].start()
    start_span(keys, k_buf, k_sem, 0)
    for load in early[1:]:
        load.start()
    for g in range(1, len(spans)):
        start_span(keys, k_buf, k_sem, g)
        start_span(values, v_buf, v_sem, g - 1)
    start_span(values, v_buf, v_sem, len(spans) - 1)
    for load in late:
        load.start()

    barrier = pltpu.get_barrier_semaphore()

    @pl.when(core == PAIR - 1)
    def _():
        for e in far:
            pl.semaphore_signal(
                barrier,
                inc=1,
                device_id={"seq": chip_at(e) * PAIR + PAIR - 1},
                device_id_type=MESH,
            )

    @pl.when(core != PAIR - 1)
    def _():
        pl.semaphore_signal(
            barrier, inc=1, device_id={"seq": chip * PAIR + PAIR - 1}, device_id_type=MESH
        )

    for e in far_first(n_head)[:-1]:
        pl.semaphore_signal(barrier, inc=1, device_id={"head": head_at(e)}, device_id_type=MESH)

    def tell_partner():
        pl.semaphore_signal(
            told, inc=1, device_id={"seq": chip * PAIR + PAIR - 1 - core}, device_id_type=MESH
        )

    diag = lax.broadcasted_iota(jnp.int32, (cands, LANES), 1) - lax.broadcasted_iota(
        jnp.int32, (cands, LANES), 0
    )

    def as_row(columns):
        spread = jnp.zeros((cands, LANES), f32)
        for k, column in columns.items():
            spread = jnp.where(diag == k * cands, column, spread)
        return jnp.sum(spread, axis=0, keepdims=True)

    def as_column(line, k):
        picked = jnp.where(diag == k * cands, line, 0.0)
        return jnp.sum(picked, axis=1, keepdims=True)

    def score(g):
        for i, e in enumerate(spans[g]):
            for c in range(PAIR):
                score_buf[e, c] = lax.dot_general(
                    q_buf[chip_at(e) * PAIR + c],
                    k_buf[g, i * PAIR + c],
                    (((1,), (1,)), ((), ())),
                    preferred_element_type=f32,
                )

    def soften(g):
        parts = {}
        for e in spans[g]:
            columns = {}
            for c in range(PAIR):
                user = chip_at(e) * PAIR + c
                scores = score_buf[e, c] * scale + bias_buf[pl.ds(user, 1), :]
                top = jnp.max(scores, axis=1, keepdims=True)
                weights = jnp.exp2(scores - top)
                parts[e, c] = weights.astype(bf16)
                columns[2 * c] = top
                columns[2 * c + 1] = jnp.sum(weights, axis=1, keepdims=True)
            send1[e, pair_rows : pair_rows + 1, :] = as_row(columns)
        return parts

    def weigh(g, parts):
        for i, e in enumerate(spans[g]):
            for c in range(PAIR):
                send1[e, c * cands : (c + 1) * cands, :] = jnp.dot(
                    parts[e, c], v_buf[g, i * PAIR + c], preferred_element_type=f32
                )

    def to_owner(e):
        return pltpu.make_async_remote_copy(
            src_ref=send1.at[e],
            dst_ref=recv1.at[e * PAIR - 1 + core if e else 0],
            send_sem=send_sem1,
            recv_sem=recv_sem1,
            device_id={"seq": chip_at(e) * PAIR + PAIR - 1},
            device_id_type=MESH,
        )

    early[0].wait()
    wait_span(keys, k_buf, k_sem, 0)
    score(0)

    for load in early[1:]:
        load.wait()
    row = lax.broadcasted_iota(jnp.int32, (users, LANES), 0)
    limit = jnp.zeros((users, LANES), jnp.int32)
    for u in range(users):
        limit = jnp.where(row == u, len_buf[u], limit)
    lane = lax.broadcasted_iota(jnp.int32, (8, LANES), 1)
    time_table, action_table = lane_table(tbias_buf[...]), lane_table(abias_buf[...])
    for r in range(0, users, 8):
        for c in range(0, block_len, LANES):
            bias = jnp.take_along_axis(
                time_table, tb_buf[r : r + 8, c : c + LANES], axis=1
            ) + jnp.take_along_axis(action_table, ac_buf[r : r + 8, c : c + LANES], axis=1)
            valid = me * block_len + c + lane < limit[r : r + 8]
            bias_buf[r : r + 8, c : c + LANES] = jnp.where(valid, bias * LOG2E, -1e30)

    for g, span in enumerate(spans):
        if g + 1 < len(spans):
            wait_span(keys, k_buf, k_sem, g + 1)
            wait_span(values, v_buf, v_sem, g)
            score(g + 1)
            parts = soften(g)
        else:
            parts = soften(g)
            wait_span(values, v_buf, v_sem, g)
        weigh(g, parts)

        if g == 0:

            @pl.when(core == PAIR - 1)
            def _():
                pl.semaphore_wait(barrier, n_chip + n_head - 1)
                tell_partner()

            @pl.when(core != PAIR - 1)
            def _():
                pl.semaphore_wait(told, 1)
                to_owner(0).start()

        for e in span:
            if e:
                to_owner(e).start()

    for load in late:
        load.wait()

    def across(e, c):
        return pltpu.make_async_remote_copy(
            src_ref=send2.at[head_at(e) * PAIR + c],
            dst_ref=recv2.at[e],
            send_sem=send_sem2,
            recv_sem=recv_sem2,
            device_id={"seq": chip * PAIR + c, "head": head_at(e)},
            device_id_type=MESH,
        )

    def arrived(buf, sem):
        pltpu.make_async_remote_copy(
            src_ref=buf,
            dst_ref=buf,
            send_sem=send_sem2,
            recv_sem=sem,
            device_id={"seq": chip * PAIR + PAIR - 1 - core},
            device_id_type=MESH,
        ).wait_recv()

    def gone(buf, sem):
        pltpu.make_async_remote_copy(
            src_ref=buf,
            dst_ref=buf,
            send_sem=sem,
            recv_sem=recv_sem2,
            device_id={"seq": chip * PAIR + PAIR - 1 - core},
            device_id_type=MESH,
        ).wait_send()

    def finish():
        whole = recv2[0]
        for e in range(1, n_head):
            whole = whole + recv2[e]
        square_sum = as_column(whole[cands : cands + 1], 0)
        factor = 1.0 / jnp.sqrt(square_sum / (width * n_head) + 1e-06)
        out[0] = (whole[:cands] * factor).astype(out.dtype)

    @pl.when(core != PAIR - 1)
    def _():
        pl.semaphore_wait(barrier, n_head - 1)
        tell_partner()
        arrived(recv2, recv_sem2)
        finish()
        gone(send1, send_sem1)

    @pl.when(core == PAIR - 1)
    def _():
        own, own_value, gated = {}, {}, {}
        for c in range(PAIR):
            own_query = q_buf[chip * PAIR + c].astype(f32)
            own[2 * c] = (
                jnp.sum(own_query * nk_buf[c].astype(f32), axis=1, keepdims=True) * scale
            )
            own_value[c] = nv_buf[c].astype(f32)
            gates = gate_buf[c].astype(f32)
            gated[c] = gain_buf[...] * (gates / (1.0 + jnp.exp(-gates)))
        own = as_row(own)
        arrived(recv1, recv_sem1)

        slots = [recv1.at[i] for i in range(n_seq - 1)] + [send1.at[0]]
        marks = jnp.zeros((n_seq, LANES), f32)
        place = lax.broadcasted_iota(jnp.int32, marks.shape, 0)
        for i, slot in enumerate(slots):
            marks = jnp.where(place == i, slot[pair_rows : pair_rows + 1, :], marks)
        overall = jnp.maximum(jnp.max(marks, axis=0, keepdims=True), own)
        factors = jnp.exp2(marks - overall)
        own_factor = jnp.exp2(own - overall)
        totals = pltpu.roll(marks, LANES - cands, 1)
        denom = own_factor + jnp.sum(factors * totals, axis=0, keepdims=True)
        hidden, squares = [], {}
        for c in range(PAIR):
            numer = as_column(own_factor, 2 * c) * own_value[c]
            for i, slot in enumerate(slots):
                numer = numer + as_column(factors[i : i + 1], 2 * c) * slot[
                    c * cands : (c + 1) * cands, :
                ]
            attended = numer / as_column(denom, 2 * c)
            squares[c] = as_row({0: jnp.sum(attended * attended, axis=1, keepdims=True)})
            hidden.append((attended * gated[c]).astype(bf16))
        hidden = jnp.concatenate(hidden, axis=0)
        for h in range(n_head):
            part = jnp.dot(
                hidden, w_buf[:, h * width : (h + 1) * width], preferred_element_type=f32
            )
            for c in range(PAIR):
                send2[h * PAIR + c, 0:cands, :] = part[c * cands : (c + 1) * cands]
                send2[h * PAIR + c, cands : cands + 1, :] = squares[c]
        heads = far_first(n_head)[:-1]
        across(heads[0], PAIR - 1).start()
        pl.semaphore_wait(told, 1)
        across(heads[0], 0).start()
        for e in heads[1:]:
            for c in range(PAIR):
                across(e, c).start()
        across(0, 0).start()
        recv2[0] = send2[my_head * PAIR + PAIR - 1]
        arrived(recv2.at[pl.ds(1, n_head - 1)], recv_sem2)
        finish()
        gone(send1.at[pl.ds(1, n_chip - 1)], send_sem1)
        gone(send2.at[pl.ds(0, n_head * PAIR - 1)], send_sem2)


def body(
    query,
    new_key,
    new_value,
    keys,
    values,
    lengths,
    time_bucket,
    action,
    time_bias,
    action_bias,
    gate,
    norm_gain,
    w_out,
):
    users, block_len, width = keys.shape
    cands = query.shape[1]
    n_seq, n_head = lax.axis_size("seq"), lax.axis_size("head")
    assert users == n_seq and width == LANES and w_out.shape[1] == n_head * width
    assert n_seq % (PAIR * SPAN) == 0 and 4 * cands <= LANES
    n_chip = n_seq // PAIR
    tile = PAIR * cands + 1
    bf16, f32, i32 = jnp.bfloat16, jnp.float32, jnp.int32
    vmem, dma = pltpu.VMEM, pltpu.SemaphoreType.DMA
    buckets, actions = time_bias.shape[0], action_bias.shape[0]
    return pl.pallas_call(
        kernel,
        name="decode",
        out_shape=pltpu.VMEM((users // n_seq, cands, width), bf16),
        in_specs=[pl.BlockSpec(memory_space=pl.ANY)] * 13,
        out_specs=pl.BlockSpec(memory_space=vmem),
        scratch_shapes=[
            vmem((users, cands, width), bf16),
            vmem((PAIR, cands, width), bf16),
            vmem((PAIR, cands, width), bf16),
            vmem((n_chip // SPAN, SPAN * PAIR, block_len, width), bf16),
            vmem((n_chip // SPAN, SPAN * PAIR, block_len, width), bf16),
            pltpu.SMEM((users,), i32),
            vmem((users, block_len), i32),
            vmem((users, block_len), i32),
            vmem((1, buckets), f32),
            vmem((1, actions), f32),
            vmem((PAIR, cands, width), bf16),
            vmem((1, width), f32),
            vmem((width, n_head * width), bf16),
            vmem((users, block_len), f32),
            vmem((n_chip, PAIR, cands, block_len), f32),
            vmem((n_chip, tile, width), f32),
            vmem((n_seq - 1, tile, width), f32),
            vmem((n_head * PAIR, cands + 1, width), f32),
            vmem((n_head, cands + 1, width), f32),
            dma((11,)),
            dma((n_chip // SPAN,)),
            dma((n_chip // SPAN,)),
            dma,
            dma,
            dma,
            dma,
            pltpu.SemaphoreType.REGULAR,
        ],
        compiler_params=pltpu.CompilerParams(collective_id=0, has_side_effects=True),
    )(
        query,
        new_key,
        new_value,
        keys,
        values,
        lengths,
        time_bucket,
        action,
        time_bias.reshape(1, buckets),
        action_bias.reshape(1, actions),
        gate,
        norm_gain.reshape(1, width),
        w_out,
    )


def solution(mesh):
    placed = (
        P("groups", None, "head"),
        P("groups", None, "head"),
        P("groups", None, "head"),
        P("groups", "seq", "head"),
        P("groups", "seq", "head"),
        P("groups"),
        P("groups", "seq"),
        P("groups", "seq"),
        P(None, "head"),
        P(None, "head"),
        P("groups", None, "head"),
        P("head"),
        P("head", None),
    )
    return jax.shard_map(
        body,
        mesh=mesh,
        in_specs=placed,
        out_specs=P(("groups", "seq"), None, "head"),
        check_vma=False,
    )
```

```python
import math

import jax
import jax.numpy as jnp
from jax import lax
from jax.experimental import pallas as pl
from jax.experimental.pallas import tpu as pltpu
from jax.sharding import PartitionSpec as P

MESH = pl.DeviceIdType.MESH
LOG2E = math.log2(math.e)
LANES = 128
PAIR = 2
SPAN = 2


def far_first(count):
    return sorted(range(count), key=lambda d: (-min(d, count - d), d))


def lane_table(table):
    rows = jnp.broadcast_to(table, (8, table.shape[1]))
    rest = LANES - table.shape[1]
    if rest:
        rows = jnp.concatenate([rows, jnp.zeros((8, rest), rows.dtype)], axis=1)
    return rows


def kernel(
    query,
    new_key,
    new_value,
    keys,
    values,
    lengths,
    time_bucket,
    action,
    time_bias,
    action_bias,
    gate,
    norm_gain,
    w_out,
    out,
    q_buf,
    nk_buf,
    nv_buf,
    k_buf,
    v_buf,
    len_buf,
    tb_buf,
    ac_buf,
    tbias_buf,
    abias_buf,
    gate_buf,
    gain_buf,
    w_buf,
    bias_buf,
    score_buf,
    send1,
    recv1,
    send2,
    recv2,
    in_sem,
    k_sem,
    v_sem,
    send_sem1,
    recv_sem1,
    send_sem2,
    recv_sem2,
    told,
    across_in,
):
    n_seq = lax.axis_size("seq")
    n_head = lax.axis_size("head")
    n_chip = n_seq // PAIR
    me = lax.axis_index("seq")
    chip, core = lax.div(me, PAIR), lax.rem(me, PAIR)
    my_head = lax.axis_index("head")
    users, cands, width = query.shape
    block_len = keys.shape[1]
    pair_rows = PAIR * cands
    scale = LOG2E / math.sqrt(width)
    far = far_first(n_chip)[:-1]
    order = list(range(n_chip))
    f32, bf16 = jnp.float32, jnp.bfloat16

    def chip_at(e):
        return lax.rem(chip + e, n_chip)

    def head_at(e):
        return lax.rem(my_head + e, n_head)

    def pair_of(source, e):
        return source.at[pl.ds(chip_at(e) * PAIR, PAIR)]

    early = [
        (query, q_buf),
        (lengths, len_buf),
        (time_bias, tbias_buf),
        (action_bias, abias_buf),
        (time_bucket, tb_buf),
        (action, ac_buf),
    ]
    late = [
        (pair_of(new_key, 0), nk_buf),
        (pair_of(new_value, 0), nv_buf),
        (pair_of(gate, 0), gate_buf),
        (norm_gain, gain_buf),
        (w_out, w_buf),
    ]
    loads = [
        pltpu.make_async_copy(src, dst, in_sem.at[i]) for i, (src, dst) in enumerate(early + late)
    ]
    early, late = loads[: len(early)], loads[len(early) :]
    spans = [order[i : i + SPAN] for i in range(0, n_chip, SPAN)]

    def start_span(source, buf, sem, g):
        for i, e in enumerate(spans[g]):
            pltpu.make_async_copy(
                pair_of(source, e), buf.at[g, pl.ds(i * PAIR, PAIR)], sem.at[g]
            ).start()

    def wait_span(source, buf, sem, g):
        pltpu.make_async_copy(source.at[pl.ds(0, SPAN * PAIR)], buf.at[g], sem.at[g]).wait()

    early[0].start()
    start_span(keys, k_buf, k_sem, 0)
    for load in early[1:]:
        load.start()
    barrier = pltpu.get_barrier_semaphore()
    half = n_chip // 2
    in_last = lax.div(chip, half)
    partner = chip * PAIR + PAIR - 1 - core

    def to_last(e):
        return chip_at(e) >= half

    pl.semaphore_signal(barrier, inc=1, device_id={"seq": partner}, device_id_type=MESH)

    @pl.when(core == PAIR - 1)
    def _():
        for e in far:
            pl.semaphore_signal(
                barrier,
                inc=1,
                device_id={"seq": chip_at(e) * PAIR + in_last},
                device_id_type=MESH,
            )

        for e in far_first(n_head)[:-1]:
            pl.semaphore_signal(
                barrier,
                inc=1,
                device_id={"seq": partner, "head": head_at(e)},
                device_id_type=MESH,
            )

    for g in range(1, len(spans)):
        start_span(keys, k_buf, k_sem, g)
        start_span(values, v_buf, v_sem, g - 1)
    start_span(values, v_buf, v_sem, len(spans) - 1)
    for load in late:
        load.start()

    def tell_partner():
        pl.semaphore_signal(told, inc=1, device_id={"seq": partner}, device_id_type=MESH)

    @pl.when(core != PAIR - 1)
    def _():
        pl.semaphore_wait(barrier, n_head + half - 1 + in_last)
        tell_partner()
        for e in far_first(n_head)[:-1]:
            pl.semaphore_signal(
                across_in,
                inc=1,
                device_id={"seq": partner, "head": head_at(e)},
                device_id_type=MESH,
            )

    diag = lax.broadcasted_iota(jnp.int32, (cands, LANES), 1) - lax.broadcasted_iota(
        jnp.int32, (cands, LANES), 0
    )

    def as_row(columns):
        spread = jnp.zeros((cands, LANES), f32)
        for k, column in columns.items():
            spread = jnp.where(diag == k * cands, column, spread)
        return jnp.sum(spread, axis=0, keepdims=True)

    def as_column(line, k):
        picked = jnp.where(diag == k * cands, line, 0.0)
        return jnp.sum(picked, axis=1, keepdims=True)

    def score(g):
        for i, e in enumerate(spans[g]):
            for c in range(PAIR):
                score_buf[e, c] = lax.dot_general(
                    q_buf[chip_at(e) * PAIR + c],
                    k_buf[g, i * PAIR + c],
                    (((1,), (1,)), ((), ())),
                    preferred_element_type=f32,
                )

    def soften(g):
        parts = {}
        for e in spans[g]:
            columns = {}
            for c in range(PAIR):
                user = chip_at(e) * PAIR + c
                scores = score_buf[e, c] * scale + bias_buf[pl.ds(user, 1), :]
                top = jnp.max(scores, axis=1, keepdims=True)
                weights = jnp.exp2(scores - top)
                parts[e, c] = weights.astype(bf16)
                columns[2 * c] = top
                columns[2 * c + 1] = jnp.sum(weights, axis=1, keepdims=True)
            send1[e, pair_rows : pair_rows + 1, :] = as_row(columns)
        return parts

    def weigh(g, parts):
        for i, e in enumerate(spans[g]):
            for c in range(PAIR):
                send1[e, c * cands : (c + 1) * cands, :] = jnp.dot(
                    parts[e, c], v_buf[g, i * PAIR + c], preferred_element_type=f32
                )

    def to_owner(e):
        return pltpu.make_async_remote_copy(
            src_ref=send1.at[e],
            dst_ref=recv1.at[e * PAIR - 1 + core if e else 0],
            send_sem=send_sem1,
            recv_sem=recv_sem1,
            device_id={"seq": chip_at(e) * PAIR + PAIR - 1},
            device_id_type=MESH,
        )

    early[0].wait()
    wait_span(keys, k_buf, k_sem, 0)
    score(0)

    for load in early[1:]:
        load.wait()
    row = lax.broadcasted_iota(jnp.int32, (users, LANES), 0)
    limit = jnp.zeros((users, LANES), jnp.int32)
    for u in range(users):
        limit = jnp.where(row == u, len_buf[u], limit)
    lane = lax.broadcasted_iota(jnp.int32, (8, LANES), 1)
    time_table, action_table = lane_table(tbias_buf[...]), lane_table(abias_buf[...])
    for r in range(0, users, 8):
        for c in range(0, block_len, LANES):
            bias = jnp.take_along_axis(
                time_table, tb_buf[r : r + 8, c : c + LANES], axis=1
            ) + jnp.take_along_axis(action_table, ac_buf[r : r + 8, c : c + LANES], axis=1)
            valid = me * block_len + c + lane < limit[r : r + 8]
            bias_buf[r : r + 8, c : c + LANES] = jnp.where(valid, bias * LOG2E, -1e30)

    for g, span in enumerate(spans):
        if g + 1 < len(spans):
            wait_span(keys, k_buf, k_sem, g + 1)
            wait_span(values, v_buf, v_sem, g)
            score(g + 1)
            parts = soften(g)
        else:
            parts = soften(g)
            wait_span(values, v_buf, v_sem, g)
        weigh(g, parts)

        if g == 0:

            @pl.when(core == PAIR - 1)
            def _():
                pl.semaphore_wait(told, 1)

            @pl.when(core != PAIR - 1)
            def _():
                to_owner(0).start()

        for e in span:
            if e:

                @pl.when(jnp.logical_not(to_last(e)))
                def _():
                    to_owner(e).start()

    def send_last():
        for e in far:

            @pl.when(to_last(e))
            def _():
                to_owner(e).start()

    @pl.when(core != PAIR - 1)
    def _():
        pl.semaphore_wait(told, 1)
        send_last()

    @pl.when(core == PAIR - 1)
    def _():
        pl.semaphore_wait(barrier, 1 + half - in_last)
        tell_partner()
        send_last()

    for load in late:
        load.wait()

    def across(e, c):
        return pltpu.make_async_remote_copy(
            src_ref=send2.at[head_at(e) * PAIR + c],
            dst_ref=recv2.at[e],
            send_sem=send_sem2,
            recv_sem=recv_sem2,
            device_id={"seq": chip * PAIR + c, "head": head_at(e)},
            device_id_type=MESH,
        )

    def arrived(buf, sem):
        pltpu.make_async_remote_copy(
            src_ref=buf,
            dst_ref=buf,
            send_sem=send_sem2,
            recv_sem=sem,
            device_id={"seq": chip * PAIR + PAIR - 1 - core},
            device_id_type=MESH,
        ).wait_recv()

    def gone(buf, sem):
        pltpu.make_async_remote_copy(
            src_ref=buf,
            dst_ref=buf,
            send_sem=sem,
            recv_sem=recv_sem2,
            device_id={"seq": chip * PAIR + PAIR - 1 - core},
            device_id_type=MESH,
        ).wait_send()

    def finish():
        whole = recv2[0]
        for e in range(1, n_head):
            whole = whole + recv2[e]
        square_sum = as_column(whole[cands : cands + 1], 0)
        factor = 1.0 / jnp.sqrt(square_sum / (width * n_head) + 1e-06)
        out[0] = (whole[:cands] * factor).astype(out.dtype)

    @pl.when(core != PAIR - 1)
    def _():
        arrived(recv2, recv_sem2)
        finish()
        gone(send1, send_sem1)

    @pl.when(core == PAIR - 1)
    def _():
        own, own_value, gated = {}, {}, {}
        for c in range(PAIR):
            own_query = q_buf[chip * PAIR + c].astype(f32)
            own[2 * c] = (
                jnp.sum(own_query * nk_buf[c].astype(f32), axis=1, keepdims=True) * scale
            )
            own_value[c] = nv_buf[c].astype(f32)
            gates = gate_buf[c].astype(f32)
            gated[c] = gain_buf[...] * (gates / (1.0 + jnp.exp(-gates)))
        own = as_row(own)
        arrived(recv1, recv_sem1)

        slots = [recv1.at[i] for i in range(n_seq - 1)] + [send1.at[0]]
        marks = jnp.zeros((n_seq, LANES), f32)
        place = lax.broadcasted_iota(jnp.int32, marks.shape, 0)
        for i, slot in enumerate(slots):
            marks = jnp.where(place == i, slot[pair_rows : pair_rows + 1, :], marks)
        overall = jnp.maximum(jnp.max(marks, axis=0, keepdims=True), own)
        factors = jnp.exp2(marks - overall)
        own_factor = jnp.exp2(own - overall)
        totals = pltpu.roll(marks, LANES - cands, 1)
        denom = own_factor + jnp.sum(factors * totals, axis=0, keepdims=True)
        hidden, squares = [], {}
        for c in range(PAIR):
            numer = as_column(own_factor, 2 * c) * own_value[c]
            for i, slot in enumerate(slots):
                numer = numer + as_column(factors[i : i + 1], 2 * c) * slot[
                    c * cands : (c + 1) * cands, :
                ]
            attended = numer / as_column(denom, 2 * c)
            squares[c] = as_row({0: jnp.sum(attended * attended, axis=1, keepdims=True)})
            hidden.append((attended * gated[c]).astype(bf16))
        hidden = jnp.concatenate(hidden, axis=0)
        for h in range(n_head):
            part = jnp.dot(
                hidden, w_buf[:, h * width : (h + 1) * width], preferred_element_type=f32
            )
            for c in range(PAIR):
                send2[h * PAIR + c, 0:cands, :] = part[c * cands : (c + 1) * cands]
                send2[h * PAIR + c, cands : cands + 1, :] = squares[c]
        heads = far_first(n_head)[:-1]
        for e in heads:
            across(e, PAIR - 1).start()

        across(0, 0).start()
        pl.semaphore_wait(across_in, n_head - 1)
        for e in heads:
            across(e, 0).start()
        recv2[0] = send2[my_head * PAIR + PAIR - 1]
        arrived(recv2.at[pl.ds(1, n_head - 1)], recv_sem2)
        finish()
        gone(send1.at[pl.ds(1, n_chip - 1)], send_sem1)
        gone(send2.at[pl.ds(0, n_head * PAIR - 1)], send_sem2)


def body(
    query,
    new_key,
    new_value,
    keys,
    values,
    lengths,
    time_bucket,
    action,
    time_bias,
    action_bias,
    gate,
    norm_gain,
    w_out,
):
    users, block_len, width = keys.shape
    cands = query.shape[1]
    n_seq, n_head = lax.axis_size("seq"), lax.axis_size("head")
    assert users == n_seq and width == LANES and w_out.shape[1] == n_head * width
    assert n_seq % (2 * PAIR * SPAN) == 0 and 4 * cands <= LANES
    n_chip = n_seq // PAIR
    tile = PAIR * cands + 1
    bf16, f32, i32 = jnp.bfloat16, jnp.float32, jnp.int32
    vmem, dma = pltpu.VMEM, pltpu.SemaphoreType.DMA
    buckets, actions = time_bias.shape[0], action_bias.shape[0]
    return pl.pallas_call(
        kernel,
        name="decode",
        out_shape=pltpu.VMEM((users // n_seq, cands, width), bf16),
        in_specs=[pl.BlockSpec(memory_space=pl.ANY)] * 13,
        out_specs=pl.BlockSpec(memory_space=vmem),
        scratch_shapes=[
            vmem((users, cands, width), bf16),
            vmem((PAIR, cands, width), bf16),
            vmem((PAIR, cands, width), bf16),
            vmem((n_chip // SPAN, SPAN * PAIR, block_len, width), bf16),
            vmem((n_chip // SPAN, SPAN * PAIR, block_len, width), bf16),
            pltpu.SMEM((users,), i32),
            vmem((users, block_len), i32),
            vmem((users, block_len), i32),
            vmem((1, buckets), f32),
            vmem((1, actions), f32),
            vmem((PAIR, cands, width), bf16),
            vmem((1, width), f32),
            vmem((width, n_head * width), bf16),
            vmem((users, block_len), f32),
            vmem((n_chip, PAIR, cands, block_len), f32),
            vmem((n_chip, tile, width), f32),
            vmem((n_seq - 1, tile, width), f32),
            vmem((n_head * PAIR, cands + 1, width), f32),
            vmem((n_head, cands + 1, width), f32),
            dma((11,)),
            dma((n_chip // SPAN,)),
            dma((n_chip // SPAN,)),
            dma,
            dma,
            dma,
            dma,
            pltpu.SemaphoreType.REGULAR,
            pltpu.SemaphoreType.REGULAR,
        ],
        compiler_params=pltpu.CompilerParams(collective_id=0, has_side_effects=True),
    )(
        query,
        new_key,
        new_value,
        keys,
        values,
        lengths,
        time_bucket,
        action,
        time_bias.reshape(1, buckets),
        action_bias.reshape(1, actions),
        gate,
        norm_gain.reshape(1, width),
        w_out,
    )


def solution(mesh):
    placed = (
        P("groups", None, "head"),
        P("groups", None, "head"),
        P("groups", None, "head"),
        P("groups", "seq", "head"),
        P("groups", "seq", "head"),
        P("groups"),
        P("groups", "seq"),
        P("groups", "seq"),
        P(None, "head"),
        P(None, "head"),
        P("groups", None, "head"),
        P("head"),
        P("head", None),
    )
    return jax.shard_map(
        body,
        mesh=mesh,
        in_specs=placed,
        out_specs=P(("groups", "seq"), None, "head"),
        check_vma=False,
    )
```

```python
import math

import jax
import jax.numpy as jnp
from jax import lax
from jax.experimental import pallas as pl
from jax.experimental.pallas import tpu as pltpu
from jax.sharding import PartitionSpec as P

MESH = pl.DeviceIdType.MESH
LOG2E = math.log2(math.e)
LANES = 128
PAIR = 2
SPAN = 2


def far_first(count):
    return sorted(range(count), key=lambda d: (-min(d, count - d), d))


def spans_of(order):
    order = list(order)
    return [order[:1], order[1:2]] + [order[i : i + SPAN] for i in range(2, len(order), SPAN)]


def tree_sum(terms):
    while len(terms) > 1:
        pairs = [a + b for a, b in zip(terms[::2], terms[1::2])]
        terms = pairs + terms[len(pairs) * 2 :]
    return terms[0]


def lane_table(table):
    rows = jnp.broadcast_to(table, (8, table.shape[1]))
    rest = LANES - table.shape[1]
    if rest:
        rows = jnp.concatenate([rows, jnp.zeros((8, rest), rows.dtype)], axis=1)
    return rows


def kernel(
    query,
    new_key,
    new_value,
    keys,
    values,
    lengths,
    time_bucket,
    action,
    time_bias,
    action_bias,
    gate,
    norm_gain,
    w_out,
    out,
    q_buf,
    nk_buf,
    nv_buf,
    k_buf,
    v_buf,
    len_buf,
    tb_buf,
    ac_buf,
    tbias_buf,
    abias_buf,
    gate_buf,
    gain_buf,
    w_buf,
    bias_buf,
    score_buf,
    send1,
    recv1,
    send2,
    recv2,
    in_sem,
    k_sem,
    v_sem,
    send_sem1,
    recv_sem1,
    send_sem2,
    recv_sem2,
    told,
    across_in,
):
    n_seq = lax.axis_size("seq")
    n_head = lax.axis_size("head")
    n_chip = n_seq // PAIR
    me = lax.axis_index("seq")
    chip, core = lax.div(me, PAIR), lax.rem(me, PAIR)
    my_head = lax.axis_index("head")
    users, cands, width = query.shape
    block_len = keys.shape[1]
    pair_rows = PAIR * cands
    scale = LOG2E / math.sqrt(width)
    far = far_first(n_chip)[:-1]
    order = sorted(range(n_chip), key=lambda e: (e + 1.5 if e == 3 else e))
    f32, bf16 = jnp.float32, jnp.bfloat16

    def chip_at(e):
        return lax.rem(chip + e, n_chip)

    def head_at(e):
        return lax.rem(my_head + e, n_head)

    def pair_of(source, e):
        return source.at[pl.ds(chip_at(e) * PAIR, PAIR)]

    early = [
        (query, q_buf),
        (lengths, len_buf),
        (time_bias, tbias_buf),
        (action_bias, abias_buf),
        (time_bucket, tb_buf),
        (action, ac_buf),
    ]
    late = [
        (pair_of(new_key, 0), nk_buf),
        (pair_of(new_value, 0), nv_buf),
        (pair_of(gate, 0), gate_buf),
        (norm_gain, gain_buf),
        (w_out, w_buf),
    ]
    loads = [
        pltpu.make_async_copy(src, dst, in_sem.at[i]) for i, (src, dst) in enumerate(early + late)
    ]
    early, late = loads[: len(early)], loads[len(early) :]
    spans = spans_of(order)
    places = {e: i * PAIR for i, e in enumerate(order)}

    def start_span(source, buf, sem, g):
        for e in spans[g]:
            pltpu.make_async_copy(
                pair_of(source, e), buf.at[pl.ds(places[e], PAIR)], sem.at[g]
            ).start()

    def wait_span(source, buf, sem, g):
        count = len(spans[g]) * PAIR
        pltpu.make_async_copy(
            source.at[pl.ds(0, count)], buf.at[pl.ds(places[spans[g][0]], count)], sem.at[g]
        ).wait()

    early[0].start()
    start_span(keys, k_buf, k_sem, 0)
    for load in early[1:]:
        load.start()
    barrier = pltpu.get_barrier_semaphore()
    half = n_chip // 2
    in_last = lax.div(chip, half)
    partner = chip * PAIR + PAIR - 1 - core

    def to_last(e):
        return chip_at(e) >= half

    pl.semaphore_signal(barrier, inc=1, device_id={"seq": partner}, device_id_type=MESH)

    @pl.when(core == PAIR - 1)
    def _():
        for e in far:
            pl.semaphore_signal(
                barrier,
                inc=1,
                device_id={"seq": chip_at(e) * PAIR + in_last},
                device_id_type=MESH,
            )

        for e in far_first(n_head)[:-1]:
            pl.semaphore_signal(
                barrier,
                inc=1,
                device_id={"seq": partner, "head": head_at(e)},
                device_id_type=MESH,
            )

    for g in range(1, len(spans)):
        start_span(keys, k_buf, k_sem, g)
        start_span(values, v_buf, v_sem, g - 1)
    start_span(values, v_buf, v_sem, len(spans) - 1)
    for load in late:
        load.start()

    def tell_partner():
        pl.semaphore_signal(told, inc=1, device_id={"seq": partner}, device_id_type=MESH)

    @pl.when(core != PAIR - 1)
    def _():
        pl.semaphore_wait(barrier, n_head + half - 1 + in_last)
        tell_partner()
        for e in far_first(n_head)[:-1]:
            pl.semaphore_signal(
                across_in.at[n_head - e],
                inc=1,
                device_id={"seq": partner, "head": head_at(e)},
                device_id_type=MESH,
            )

    diag = lax.broadcasted_iota(jnp.int32, (cands, LANES), 1) - lax.broadcasted_iota(
        jnp.int32, (cands, LANES), 0
    )

    def as_row(columns):
        spread = jnp.zeros((cands, LANES), f32)
        for k, column in columns.items():
            spread = jnp.where(diag == k * cands, column, spread)
        return jnp.sum(spread, axis=0, keepdims=True)

    def as_column(line, k):
        picked = jnp.where(diag == k * cands, line, 0.0)
        return jnp.sum(picked, axis=1, keepdims=True)

    def score(g):
        for e in spans[g]:
            for c in range(PAIR):
                score_buf[e, c] = lax.dot_general(
                    q_buf[chip_at(e) * PAIR + c],
                    k_buf[places[e] + c],
                    (((1,), (1,)), ((), ())),
                    preferred_element_type=f32,
                )

    def soften(g):
        parts = {}
        for e in spans[g]:
            columns = {}
            for c in range(PAIR):
                user = chip_at(e) * PAIR + c
                scores = score_buf[e, c] * scale + bias_buf[pl.ds(user, 1), :]
                top = jnp.max(scores, axis=1, keepdims=True)
                weights = jnp.exp2(scores - top)
                parts[e, c] = weights.astype(bf16)
                columns[2 * c] = top
                columns[2 * c + 1] = jnp.sum(weights, axis=1, keepdims=True)
            send1[e, pair_rows : pair_rows + 1, :] = as_row(columns)
        return parts

    def weigh(g, parts):
        for e in spans[g]:
            for c in range(PAIR):
                send1[e, c * cands : (c + 1) * cands, :] = jnp.dot(
                    parts[e, c], v_buf[places[e] + c], preferred_element_type=f32
                )

    def to_owner(e):
        return pltpu.make_async_remote_copy(
            src_ref=send1.at[e],
            dst_ref=recv1.at[e * PAIR - 1 + core if e else 0],
            send_sem=send_sem1,
            recv_sem=recv_sem1,
            device_id={"seq": chip_at(e) * PAIR + PAIR - 1},
            device_id_type=MESH,
        )

    early[0].wait()
    wait_span(keys, k_buf, k_sem, 0)
    score(0)

    for load in early[1:]:
        load.wait()
    row = lax.broadcasted_iota(jnp.int32, (users, LANES), 0)
    limit = jnp.zeros((users, LANES), jnp.int32)
    for u in range(users):
        limit = jnp.where(row == u, len_buf[u], limit)
    lane = lax.broadcasted_iota(jnp.int32, (8, LANES), 1)
    time_table, action_table = lane_table(tbias_buf[...]), lane_table(abias_buf[...])
    for r in range(0, users, 8):
        for c in range(0, block_len, LANES):
            bias = jnp.take_along_axis(
                time_table, tb_buf[r : r + 8, c : c + LANES], axis=1
            ) + jnp.take_along_axis(action_table, ac_buf[r : r + 8, c : c + LANES], axis=1)
            valid = me * block_len + c + lane < limit[r : r + 8]
            bias_buf[r : r + 8, c : c + LANES] = jnp.where(valid, bias * LOG2E, -1e30)

    for g, span in enumerate(spans):
        if g + 1 < len(spans):
            wait_span(keys, k_buf, k_sem, g + 1)
            wait_span(values, v_buf, v_sem, g)
            score(g + 1)
            parts = soften(g)
        else:
            parts = soften(g)
            wait_span(values, v_buf, v_sem, g)
        weigh(g, parts)

        if g == 0:

            @pl.when(core == PAIR - 1)
            def _():
                pl.semaphore_wait(told, 1)

            @pl.when(core != PAIR - 1)
            def _():
                to_owner(0).start()

        for e in span:
            if e:

                @pl.when(jnp.logical_not(to_last(e)))
                def _():
                    to_owner(e).start()

    def send_last():
        for e in far:

            @pl.when(to_last(e))
            def _():
                to_owner(e).start()

    @pl.when(core != PAIR - 1)
    def _():
        pl.semaphore_wait(told, 1)
        send_last()

    @pl.when(core == PAIR - 1)
    def _():
        pl.semaphore_wait(barrier, 1 + half - in_last)
        tell_partner()
        send_last()

    for load in late:
        load.wait()

    def across(e, c):
        return pltpu.make_async_remote_copy(
            src_ref=send2.at[head_at(e) * PAIR + c],
            dst_ref=recv2.at[e],
            send_sem=send_sem2,
            recv_sem=recv_sem2,
            device_id={"seq": chip * PAIR + c, "head": head_at(e)},
            device_id_type=MESH,
        )

    def arrived(buf, sem):
        pltpu.make_async_remote_copy(
            src_ref=buf,
            dst_ref=buf,
            send_sem=send_sem2,
            recv_sem=sem,
            device_id={"seq": chip * PAIR + PAIR - 1 - core},
            device_id_type=MESH,
        ).wait_recv()

    def gone(buf, sem):
        pltpu.make_async_remote_copy(
            src_ref=buf,
            dst_ref=buf,
            send_sem=sem,
            recv_sem=recv_sem2,
            device_id={"seq": chip * PAIR + PAIR - 1 - core},
            device_id_type=MESH,
        ).wait_send()

    def finish():
        whole = tree_sum([recv2[e] for e in range(n_head)])
        square_sum = as_column(whole[cands : cands + 1], 0)
        factor = 1.0 / jnp.sqrt(square_sum / (width * n_head) + 1e-06)
        out[0] = (whole[:cands] * factor).astype(out.dtype)

    @pl.when(core != PAIR - 1)
    def _():
        arrived(recv2, recv_sem2)
        finish()
        gone(send1, send_sem1)

    @pl.when(core == PAIR - 1)
    def _():
        own, own_value, gated = {}, {}, {}
        for c in range(PAIR):
            own_query = q_buf[chip * PAIR + c].astype(f32)
            own[2 * c] = (
                jnp.sum(own_query * nk_buf[c].astype(f32), axis=1, keepdims=True) * scale
            )
            own_value[c] = nv_buf[c].astype(f32)
            gates = gate_buf[c].astype(f32)
            gated[c] = gain_buf[...] * (gates / (1.0 + jnp.exp(-gates)))
        own = as_row(own)
        arrived(recv1, recv_sem1)

        slots = [recv1.at[i] for i in range(n_seq - 1)] + [send1.at[0]]
        marks = jnp.zeros((n_seq, LANES), f32)
        place = lax.broadcasted_iota(jnp.int32, marks.shape, 0)
        for i, slot in enumerate(slots):
            marks = jnp.where(place == i, slot[pair_rows : pair_rows + 1, :], marks)
        overall = jnp.maximum(jnp.max(marks, axis=0, keepdims=True), own)
        factors = jnp.exp2(marks - overall)
        own_factor = jnp.exp2(own - overall)
        totals = pltpu.roll(marks, LANES - cands, 1)
        denom = own_factor + jnp.sum(factors * totals, axis=0, keepdims=True)
        hidden, squares = [], {}
        for c in range(PAIR):
            terms = [as_column(own_factor, 2 * c) * own_value[c]]
            for i, slot in enumerate(slots):
                rows = slot[c * cands : (c + 1) * cands, :]
                terms.append(as_column(factors[i : i + 1], 2 * c) * rows)
            attended = tree_sum(terms) / as_column(denom, 2 * c)
            squares[c] = as_row({0: jnp.sum(attended * attended, axis=1, keepdims=True)})
            hidden.append((attended * gated[c]).astype(bf16))
        hidden = jnp.concatenate(hidden, axis=0)
        for h in range(n_head):
            part = jnp.dot(
                hidden, w_buf[:, h * width : (h + 1) * width], preferred_element_type=f32
            )
            for c in range(PAIR):
                send2[h * PAIR + c, 0:cands, :] = part[c * cands : (c + 1) * cands]
                send2[h * PAIR + c, cands : cands + 1, :] = squares[c]
        heads = far_first(n_head)[:-1]
        heads = [heads[0]] + sorted(heads[1:], key=lambda e: e != 1)
        for e in heads[:2]:
            across(e, PAIR - 1).start()
        pl.semaphore_wait(across_in.at[1], 1)
        across(1, 0).start()
        for e in heads[2:]:
            across(e, PAIR - 1).start()
        across(0, 0).start()
        for e in heads:
            if e != 1:
                pl.semaphore_wait(across_in.at[e], 1)
                across(e, 0).start()
        recv2[0] = send2[my_head * PAIR + PAIR - 1]
        arrived(recv2.at[pl.ds(1, n_head - 1)], recv_sem2)
        finish()
        gone(send1.at[pl.ds(1, n_chip - 1)], send_sem1)
        gone(send2.at[pl.ds(0, n_head * PAIR - 1)], send_sem2)


def body(
    query,
    new_key,
    new_value,
    keys,
    values,
    lengths,
    time_bucket,
    action,
    time_bias,
    action_bias,
    gate,
    norm_gain,
    w_out,
):
    users, block_len, width = keys.shape
    cands = query.shape[1]
    n_seq, n_head = lax.axis_size("seq"), lax.axis_size("head")
    assert users == n_seq and width == LANES and w_out.shape[1] == n_head * width
    assert n_seq % (2 * PAIR * SPAN) == 0 and 4 * cands <= LANES
    n_chip = n_seq // PAIR
    tile = PAIR * cands + 1
    bf16, f32, i32 = jnp.bfloat16, jnp.float32, jnp.int32
    vmem, dma = pltpu.VMEM, pltpu.SemaphoreType.DMA
    buckets, actions = time_bias.shape[0], action_bias.shape[0]
    return pl.pallas_call(
        kernel,
        name="decode",
        out_shape=pltpu.VMEM((users // n_seq, cands, width), bf16),
        in_specs=[pl.BlockSpec(memory_space=pl.ANY)] * 13,
        out_specs=pl.BlockSpec(memory_space=vmem),
        scratch_shapes=[
            vmem((users, cands, width), bf16),
            vmem((PAIR, cands, width), bf16),
            vmem((PAIR, cands, width), bf16),
            vmem((users, block_len, width), bf16),
            vmem((users, block_len, width), bf16),
            pltpu.SMEM((users,), i32),
            vmem((users, block_len), i32),
            vmem((users, block_len), i32),
            vmem((1, buckets), f32),
            vmem((1, actions), f32),
            vmem((PAIR, cands, width), bf16),
            vmem((1, width), f32),
            vmem((width, n_head * width), bf16),
            vmem((users, block_len), f32),
            vmem((n_chip, PAIR, cands, block_len), f32),
            vmem((n_chip, tile, width), f32),
            vmem((n_seq - 1, tile, width), f32),
            vmem((n_head * PAIR, cands + 1, width), f32),
            vmem((n_head, cands + 1, width), f32),
            dma((11,)),
            dma((len(spans_of(range(n_chip))),)),
            dma((len(spans_of(range(n_chip))),)),
            dma,
            dma,
            dma,
            dma,
            pltpu.SemaphoreType.REGULAR,
            pltpu.SemaphoreType.REGULAR((n_head,)),
        ],
        compiler_params=pltpu.CompilerParams(collective_id=0, has_side_effects=True),
    )(
        query,
        new_key,
        new_value,
        keys,
        values,
        lengths,
        time_bucket,
        action,
        time_bias.reshape(1, buckets),
        action_bias.reshape(1, actions),
        gate,
        norm_gain.reshape(1, width),
        w_out,
    )


def solution(mesh):
    placed = (
        P("groups", None, "head"),
        P("groups", None, "head"),
        P("groups", None, "head"),
        P("groups", "seq", "head"),
        P("groups", "seq", "head"),
        P("groups"),
        P("groups", "seq"),
        P("groups", "seq"),
        P(None, "head"),
        P(None, "head"),
        P("groups", None, "head"),
        P("head"),
        P("head", None),
    )
    return jax.shard_map(
        body,
        mesh=mesh,
        in_specs=placed,
        out_specs=P(("groups", "seq"), None, "head"),
        check_vma=False,
    )
```
